512 devices in a mesh: gx: 8 (over z), gy: 8 (over y), gz: 8 (over x, core).
Axes of the slice: x: 4, y: 8, z: 8, core: 2. Of those that a mesh axis runs over, the one named last changes fastest.
Arguments:
- strain: float32 [2, 4, 128, 128, 1024], P(None, None, 'gx', 'gy', 'gz'), may hold values from -6 to 6
- cell_shell_index: int32 [128, 128, 1024], P('gx', 'gy', 'gz'), may hold values from 0 to 255
- onset_step: int32 [256], replicated, may hold values from 0 to 1
Outputs:
- psi_four: float32 [2, 4, 128, 128, 1024], P(None, None, 'gx', 'gy', 'gz')
- energy: float32 [8, 4, 256], P('gx', None, ('gy', 'gz'))
The draws below stay inside these ranges and needn't reach their ends.
All inputs are finite; a program needn't handle non-finite values.
Results may differ from the reference program's by a relative error of at most 0.00007.
Values sent between devices are 32-bit elements; how exact they have to be, the bound alone decides.
A program may use at most 64 MiB of HBM per device.

```python
import jax
import jax.numpy as jnp
from jax import lax

CX = 16
NT = 4
SHELLS = 256
NX = 128
NY = 128
NZ = 1024
N_GX = 8


def set_ends(values, stream_key, smallest, largest):
    index_at = [jax.random.randint(jax.random.fold_in(stream_key, axis), (), 0, length) for axis, length in enumerate(values.shape)]
    main_axis = values.shape.index(max(values.shape))
    beside = index_at[:main_axis] + [(index_at[main_axis] + 1) % values.shape[main_axis]] + index_at[main_axis + 1:]
    return values.at[tuple(index_at)].set(smallest).at[tuple(beside)].set(largest)


def block_levels(own_key, dims, pieces, least, high):
    loudness, own = 1.0, jax.random.fold_in(own_key, 6)
    for position, shards_of in pieces:
        heights = jnp.exp(jax.random.uniform(jax.random.fold_in(own, position), (shards_of,), jnp.float32, least / len(pieces), high / len(pieces)))
        loudness = loudness * jnp.repeat(heights, dims[position] // shards_of).reshape([-1 if axis == position else 1 for axis in range(len(dims))])
    return loudness


def centred(rng, extent, spread, limit, split=(), held_as=jnp.bfloat16):
    array = jax.random.normal(rng, extent, jnp.float32) * spread
    if len(split) > 0:
        array = block_levels(rng, extent, split, -0.22, 0.18) * array
    return jnp.clip(array, min=-limit, max=limit).astype(held_as)


def setup_inputs(seed: int = 0) -> dict:
    keys = jax.random.split(jax.random.key(seed), 4)
    strain = centred(keys[0], (2, NT, NX, NY, NZ), 1.0, 6.0, ((2, 8), (3, 8), (4, 8)), jnp.float32)
    cell_shell_index = set_ends(jax.random.randint(keys[1], (NX, NY, NZ), 0, SHELLS), jax.random.fold_in(keys[1], 1), 0, SHELLS - 1).astype(jnp.int32)
    onset_step = set_ends(jax.random.randint(keys[2], (SHELLS,), 0, NT // 2), jax.random.fold_in(keys[2], 1), 0, (NT // 2) - 1).astype(jnp.int32)
    return dict(strain=strain, cell_shell_index=cell_shell_index, onset_step=onset_step)


first_coef = ((-2, 1.0), (-1, -8.0), (1, 8.0), (2, -1.0))
second_coef = ((-2, -1.0), (-1, 16.0), (0, -30.0), (1, 16.0), (2, -1.0))


def take_shifted(padded, off_x, off_y, off_z):
    len_x = padded.shape[2] - 4
    len_y = padded.shape[3] - 4
    len_z = padded.shape[4] - 4
    return padded[:, :, 2 + off_x:2 + off_x + len_x, 2 + off_y:2 + off_y + len_y, 2 + off_z:2 + off_z + len_z]


def reference(strain, cell_shell_index, onset_step):
    padded = jnp.pad(strain, ((0, 0), (0, 0), (2, 2), (2, 2), (2, 2)))
    second_x = sum(w * take_shifted(padded, k, 0, 0) for k, w in second_coef) / 12.0
    second_y = sum(w * take_shifted(padded, 0, k, 0) for k, w in second_coef) / 12.0
    second_z = sum(w * take_shifted(padded, 0, 0, k) for k, w in second_coef) / 12.0
    mixed_yz = sum(wa * wb * take_shifted(padded, 0, ka, kb) for ka, wa in first_coef for kb, wb in first_coef) / 144.0
    combo = second_x + second_y - second_z
    real_part = 0.5 * combo[0] - mixed_yz[1]
    imag_part = -0.5 * combo[1] - mixed_yz[0]
    psi_four = jnp.stack([real_part, imag_part])
    bondi_news = jnp.cumsum(psi_four, axis=1) * 0.25
    position_along_x = (jnp.arange(NX, dtype=jnp.float32) + 0.5) / NX - 0.5
    position_along_y = (jnp.arange(NY, dtype=jnp.float32) + 0.5) / NY - 0.5
    position_along_z = (jnp.arange(NZ, dtype=jnp.float32) + 0.5) / NZ - 0.5
    radius_squared = position_along_x[:, None, None] ** 2 + position_along_y[None, :, None] ** 2 + position_along_z[None, None, :] ** 2 + 0.05
    energy_flux = radius_squared[None] * (bondi_news[0] ** 2 + bondi_news[1] ** 2)
    flux_slabs = energy_flux.reshape(NT, N_GX, CX * NY * NZ)
    id_slabs = cell_shell_index.reshape(N_GX, CX * NY * NZ)

    def per_slab(slab):
        data = lax.dynamic_index_in_dim(flux_slabs, slab, 1, keepdims=False)
        ids = lax.dynamic_index_in_dim(id_slabs, slab, 0, keepdims=False)
        return jax.ops.segment_sum(data.T, ids, num_segments=SHELLS).T

    binned = lax.map(per_slab, jnp.arange(N_GX, dtype=jnp.int32))
    live = (jnp.arange(NT, dtype=jnp.int32)[:, None] >= onset_step[None, :]).astype(jnp.float32)
    binned = binned * live[None]
    scale = 0.25 * SHELLS / (NX * NY * NZ)
    energy = jnp.cumsum(jnp.cumsum(binned, axis=1), axis=0) * scale
    return psi_four, energy
```

```python
import jax
import jax.numpy as jnp
from jax import lax
from jax.experimental import pallas as pl
from jax.experimental.pallas import tpu as pltpu
from jax.sharding import PartitionSpec as P

MESH = pl.DeviceIdType.MESH
F32 = jnp.float32


def kernel(
    sizes,
    strain,
    shells,
    onset,
    psi_out,
    energy_out,
    field,
    shell,
    onsets,
    zpack,
    zlow,
    zhigh,
    firsts,
    seconds,
    psi,
    binned,
    parts,
    got_y,
    got_z,
    got_x,
    total_yz,
    in_sem,
    out_sem,
    halo_send,
    halo_recv,
    sum_send,
    sum_recv,
):
    nx, ny, nz = sizes
    gx, gy, gz = (lax.axis_index(a) for a in ("gx", "gy", "gz"))
    cx = 16
    ct = 8

    loads = [
        pltpu.make_async_copy(strain.at[c], field.at[2:18, 2:18, c], in_sem.at[c]) for c in range(ct)
    ]
    loads.append(pltpu.make_async_copy(shells, shell, in_sem.at[ct]))
    loads.append(pltpu.make_async_copy(onset, onsets, in_sem.at[ct + 1]))
    for load in loads:
        load.start()

    below = {"gx": gx > 0, "gy": gy > 0, "gz": gz > 0}
    above = {"gx": gx < nx - 1, "gy": gy < ny - 1, "gz": gz < nz - 1}
    at = {"gx": gx, "gy": gy, "gz": gz}
    count = {"gx": nx, "gy": ny, "gz": nz}

    barrier = pltpu.get_barrier_semaphore()
    for axis in ("gx", "gy", "gz"):
        for d in range(1, count[axis]):
            pl.semaphore_signal(
                barrier,
                inc=1,
                device_id={axis: lax.rem(at[axis] + d, count[axis])},
                device_id_type=MESH,
            )
    corners = []
    for has_y, step_y in ((below["gy"], -1), (above["gy"], 1)):
        for has_z, step_z in ((below["gz"], -1), (above["gz"], 1)):
            both = jnp.logical_and(has_y, has_z)
            corners.append((both, {"gy": gy + step_y, "gz": gz + step_z}))
    for both, peer in corners:

        @pl.when(both)
        def _(peer=peer):
            pl.semaphore_signal(barrier, inc=1, device_id=peer, device_id_type=MESH)

    greeted = nx - 1 + ny - 1 + nz - 1
    for both, _ in corners:
        greeted = greeted + both.astype(jnp.int32)

    def zero(where, ref):
        @pl.when(where)
        def _():
            ref[...] = jnp.zeros(ref.shape, F32)

    no = jnp.logical_not
    zero(no(below["gx"]), field.at[0:2, 2:18])
    zero(no(above["gx"]), field.at[18:20, 2:18])
    zero(no(below["gy"]), field.at[2:18, 0:2])
    zero(no(above["gy"]), field.at[2:18, 18:20])
    zero(no(below["gz"]), zlow.at[1:9])
    zero(no(above["gz"]), zhigh.at[1:9])
    zero(no(corners[0][0]), zlow.at[0])
    zero(no(corners[1][0]), zhigh.at[0])
    zero(no(corners[2][0]), zlow.at[9])
    zero(no(corners[3][0]), zhigh.at[9])

    lane = lax.broadcasted_iota(jnp.int32, (8, 128), 1)
    sub = lax.broadcasted_iota(jnp.int32, (8, 128), 0)
    slot_of = ((lane + 2) & 127) >> 2

    for load in loads:
        load.wait()

    def pack(x, acc):
        acc = list(acc)
        for b in range(8):
            for p in range(2):
                slot = 2 * x + p
                moved = pltpu.roll(field[x + 2, 2 * b + p + 2], 4 * slot, 1)
                acc[b] = jnp.where(slot_of == slot, moved, acc[b])
        return tuple(acc)

    packed = lax.fori_loop(0, cx, pack, tuple(jnp.zeros((8, 128), F32) for _ in range(8)))
    for b in range(8):
        zpack[b] = packed[b]

    pl.semaphore_wait(barrier, greeted)

    def halo(i, has, src, dst, peer, sends):
        copy = pltpu.make_async_remote_copy(
            src_ref=src,
            dst_ref=dst,
            send_sem=halo_send.at[i],
            recv_sem=halo_recv.at[i],
            device_id=peer,
            device_id_type=MESH,
        )
        sends.append((has, copy))

    sends = []
    halo(0, above["gz"], zpack, zlow.at[1:9], {"gz": gz + 1}, sends)
    halo(1, below["gz"], zpack, zhigh.at[1:9], {"gz": gz - 1}, sends)
    halo(2, corners[3][0], zpack.at[7], zlow.at[0], corners[3][1], sends)
    halo(3, corners[2][0], zpack.at[7], zhigh.at[0], corners[2][1], sends)
    halo(4, corners[1][0], zpack.at[0], zlow.at[9], corners[1][1], sends)
    halo(5, corners[0][0], zpack.at[0], zhigh.at[9], corners[0][1], sends)
    halo(6, above["gy"], field.at[2:18, 16:18], field.at[2:18, 0:2], {"gy": gy + 1}, sends)
    halo(7, below["gy"], field.at[2:18, 2:4], field.at[2:18, 18:20], {"gy": gy - 1}, sends)
    halo(8, above["gx"], field.at[16:18, 2:18], field.at[0:2, 2:18], {"gx": gx + 1}, sends)
    halo(9, below["gx"], field.at[2:4, 2:18], field.at[18:20, 2:18], {"gx": gx - 1}, sends)
    arrives = [
        below["gz"],
        above["gz"],
        corners[0][0],
        corners[1][0],
        corners[2][0],
        corners[3][0],
        below["gy"],
        above["gy"],
        below["gx"],
        above["gx"],
    ]
    for has, copy in sends:

        @pl.when(has)
        def _(copy=copy):
            copy.start()

    def arrive(i):
        @pl.when(arrives[i])
        def _():
            sends[i][1].wait_recv()

    for i in range(6):
        arrive(i)

    def along_z(ys):
        edges = {b: jnp.where((lane & 2) != 0, zlow[b], zhigh[b]) for b in sorted({y // 2 for y in ys})}

        def step(x, _):
            for y in ys:
                f = field[x + 2, y]
                end = pltpu.roll(edges[y // 2], 128 - 4 * (2 * x + y % 2), 1)
                up1 = pltpu.roll(jnp.where(lane >= 1, f, end), 127, 1)
                up2 = pltpu.roll(jnp.where(lane >= 2, f, end), 126, 1)
                down1 = pltpu.roll(jnp.where(lane < 127, f, end), 1, 1)
                down2 = pltpu.roll(jnp.where(lane < 126, f, end), 2, 1)
                firsts[x, y] = 8.0 * (up1 - down1) - (up2 - down2)
                if 2 <= y < 18:
                    seconds[x, y - 2] = 16.0 * (up1 + down1) - (up2 + down2)
            return 0

        lax.fori_loop(0, cx, step, 0)

    along_z(list(range(2, 18)))
    for i in range(6, 10):
        arrive(i)
    along_z([0, 1, 18, 19])

    signs = jnp.where(sub < 4, 1.0 / 24.0, -1.0 / 24.0).astype(F32)
    step_of = sub & 3
    uz = (lane + gz * 128).astype(F32)
    uz = (uz + 0.5) / (nz * 128) - 0.5
    uz2 = uz * uz + 0.05

    def main(x, total):
        ux = (x + gx * cx).astype(F32)
        ux = (ux + 0.5) / (nx * cx) - 0.5
        ux2 = uz2 + ux * ux
        lefts, rights = [], []
        for y in range(16):
            f = field[x + 2, y + 2]
            near = (field[x + 1, y + 2] + field[x + 3, y + 2]) + (field[x + 2, y + 1] + field[x + 2, y + 3])
            far = (field[x, y + 2] + field[x + 4, y + 2]) + (field[x + 2, y] + field[x + 2, y + 4])
            combo = (16.0 * near - far) - (seconds[x, y] + 30.0 * f)
            mixed = 8.0 * (firsts[x, y + 3] - firsts[x, y + 1]) - (firsts[x, y + 4] - firsts[x, y])
            value = combo * signs - pltpu.roll(mixed, 4, 0) * (1.0 / 144.0)
            psi[x, y] = value
            news = value + jnp.where(step_of >= 1, pltpu.roll(value, 1, 0), 0.0)
            news = news + jnp.where(step_of >= 2, pltpu.roll(news, 2, 0), 0.0)
            power = news * news
            power = power + pltpu.roll(power, 4, 0)
            uy = (gy * 16 + y).astype(F32)
            uy = (uy + 0.5) / (ny * 16) - 0.5
            flux = power * ((ux2 + uy * uy) * 0.0625)
            high = flux.astype(jnp.bfloat16).astype(F32)
            split = jnp.where(sub < 4, high, flux - high)
            label = jnp.broadcast_to(shell[x, pl.ds(y, 1), :], (8, 128))
            outer = label >> 5
            inner = label & 31
            lefts.append(jnp.concatenate([jnp.where(outer == k, split, 0.0) for k in range(8)], axis=0))
            rights.append(
                jnp.concatenate([jnp.where(inner == sub + 8 * j, 1.0, 0.0).astype(F32) for j in range(4)], axis=0)
            )
        left = jnp.concatenate(lefts, axis=1)
        right = jnp.concatenate(rights, axis=1)
        return total + lax.dot_general(
            left, right, (((1,), (1,)), ((), ())), preferred_element_type=F32
        )

    total = lax.fori_loop(0, cx, main, jnp.zeros((64, 32), F32))

    stores = [
        pltpu.make_async_copy(psi.at[:, :, c], psi_out.at[c], out_sem.at[c]) for c in range(ct)
    ]
    for store in stores:
        store.start()

    def by_step(x, moves):
        moved = x
        for t in range(1, 4):
            moved = jnp.where(step_of == t, pltpu.roll(x, moves[t], 1), moved)
        return moved

    binned[...] = jnp.zeros((64, 128), F32)
    binned[:, 0:32] = total
    for k in range(8):
        spread = by_step(binned[8 * k : 8 * k + 8, :], (0, 32, 64, 96))
        parts[k] = jnp.sum(spread, axis=0, keepdims=True)

    def exchange(axis, base, src, dst, use):
        me, n = at[axis], count[axis]
        copies = []
        for d in range(1, n):
            peer = lax.rem(me + d, n)
            copies.append(
                pltpu.make_async_remote_copy(
                    src_ref=src(peer),
                    dst_ref=dst.at[d],
                    send_sem=sum_send.at[base + d],
                    recv_sem=sum_recv.at[base + d],
                    device_id={axis: peer},
                    device_id_type=MESH,
                )
            )
        for copy in copies:
            copy.start()
        for copy in copies:
            copy.wait_recv()
        result = use(dst)
        return copies, result

    def summed(own):
        def use(dst):
            value = own
            for d in range(1, 8):
                value = value + dst[d]
            return value

        return use

    copies_y, sum_y = exchange("gy", 0, lambda peer: parts.at[peer], got_y, summed(parts[gy]))
    total_yz[0] = sum_y
    copies_z, sum_z = exchange("gz", 8, lambda peer: total_yz.at[0], got_z, summed(sum_y))
    total_yz[1] = sum_z

    def lower(dst):
        value = sum_z
        for d in range(1, 8):
            value = value + jnp.where(gx >= d, dst[d], 0.0)
        return value

    copies_x, sum_x = exchange("gx", 16, lambda peer: total_yz.at[1], got_x, lower)

    first = jnp.broadcast_to(onsets[pl.ds(gy // 4, 1), :], (8, 128))
    first = pltpu.roll(first, lax.rem(128 - 32 * lax.rem(gy, 4), 128), 1)
    first = jnp.where(lane < 32, first, 0)
    first = first + pltpu.roll(first, 32, 1)
    first = first + pltpu.roll(first, 64, 1)
    value = jnp.broadcast_to(sum_x, (8, 128))
    value = jnp.where((lane >> 5) >= first, value, 0.0)
    value = value + jnp.where(lane >= 32, pltpu.roll(value, 32, 1), 0.0)
    value = value + jnp.where(lane >= 64, pltpu.roll(value, 64, 1), 0.0)
    value = value * (0.25 * 256 / (nx * 16 * ny * 16 * nz * 128))
    value = pltpu.roll(value, lax.rem(128 - 4 * gz, 128), 1)
    value = by_step(value, (0, 96, 64, 32))
    energy_out[0] = value[0:4, 0:4]

    for has, copy in sends:

        @pl.when(has)
        def _(copy=copy):
            copy.wait_send()

    for copy in copies_y + copies_z + copies_x:
        copy.wait_send()
    for store in stores:
        store.wait()


def solution(mesh):
    sizes = tuple(mesh.shape[a] for a in ("gx", "gy", "gz"))

    def body(strain, cell_shell_index, onset_step):
        run = pl.pallas_call(
            lambda *refs: kernel(sizes, *refs),
            out_shape=(
                jax.ShapeDtypeStruct((8, 16, 16, 128), F32),
                jax.ShapeDtypeStruct((1, 4, 4), F32),
            ),
            in_specs=[pl.BlockSpec(memory_space=pltpu.HBM)] * 3,
            out_specs=(
                pl.BlockSpec(memory_space=pltpu.HBM),
                pl.BlockSpec(memory_space=pltpu.VMEM),
            ),
            scratch_shapes=[
                pltpu.VMEM((20, 20, 8, 128), F32),
                pltpu.VMEM((16, 16, 128), jnp.int32),
                pltpu.VMEM((2, 128), jnp.int32),
                pltpu.VMEM((8, 8, 128), F32),
                pltpu.VMEM((10, 8, 128), F32),
                pltpu.VMEM((10, 8, 128), F32),
                pltpu.VMEM((16, 20, 8, 128), F32),
                pltpu.VMEM((16, 16, 8, 128), F32),
                pltpu.VMEM((16, 16, 8, 128), F32),
                pltpu.VMEM((64, 128), F32),
                pltpu.VMEM((8, 1, 128), F32),
                pltpu.VMEM((8, 1, 128), F32),
                pltpu.VMEM((8, 1, 128), F32),
                pltpu.VMEM((8, 1, 128), F32),
                pltpu.VMEM((2, 1, 128), F32),
                pltpu.SemaphoreType.DMA((10,)),
                pltpu.SemaphoreType.DMA((8,)),
                pltpu.SemaphoreType.DMA((10,)),
                pltpu.SemaphoreType.DMA((10,)),
                pltpu.SemaphoreType.DMA((24,)),
                pltpu.SemaphoreType.DMA((24,)),
            ],
            compiler_params=pltpu.CompilerParams(collective_id=0, has_side_effects=True),
        )
        psi_four, energy = run(
            strain.reshape(8, 16, 16, 128), cell_shell_index, onset_step.reshape(2, 128)
        )
        return psi_four.reshape(strain.shape), energy

    placed = (P(None, None, "gx", "gy", "gz"), P("gx", "gy", "gz"), P())
    return jax.shard_map(
        body,
        mesh=mesh,
        in_specs=placed,
        out_specs=(P(None, None, "gx", "gy", "gz"), P("gx", None, ("gy", "gz"))),
        check_vma=False,
    )
```

```python
import jax
import jax.numpy as jnp
from jax import lax
from jax.experimental import pallas as pl
from jax.experimental.pallas import tpu as pltpu
from jax.sharding import PartitionSpec as P

MESH = pl.DeviceIdType.MESH
F32 = jnp.float32
CT = 8


def kernel(
    sizes,
    strain,
    shells,
    onset,
    psi_out,
    energy_out,
    field,
    shell,
    onsets,
    zmid,
    zlow,
    zhigh,
    edge,
    firsts,
    seconds,
    binned,
    parts,
    got_y,
    got_z,
    got_x,
    summed,
    in_sem,
    halo_send,
    halo_recv,
    sum_send,
    sum_recv,
    know,
):
    nx, ny, nz = sizes
    gx, gy, gz = (lax.axis_index(a) for a in ("gx", "gy", "gz"))
    no = jnp.logical_not
    both = jnp.logical_and

    loads = [
        pltpu.make_async_copy(strain.at[c], field.at[2:18, 2:18, c], in_sem.at[c]) for c in range(CT)
    ]
    loads.append(pltpu.make_async_copy(shells, shell, in_sem.at[CT]))
    loads.append(pltpu.make_async_copy(onset, onsets, in_sem.at[CT + 1]))
    for load in loads:
        load.start()

    def when(cond, act):
        if cond is None:
            act()
        else:
            pl.when(cond)(act)

    def tell(sem, peer, cond=None):
        when(cond, lambda: pl.semaphore_signal(sem, inc=1, device_id=peer, device_id_type=MESH))

    def hear(sem, cond=None):
        when(cond, lambda: pl.semaphore_wait(sem, 1))

    def ring(axis, step):
        n = {"gy": ny, "gz": nz}[axis]
        return {axis: lax.rem({"gy": gy, "gz": gz}[axis] + (step + n), n)}

    barrier = pltpu.get_barrier_semaphore()
    x_lo, x_hi = gx > 0, gx < nx - 1
    y_lo, y_hi = gy > 0, gy < ny - 1
    z_lo, z_hi = gz > 0, gz < nz - 1
    tell(barrier, {"gx": gx - 1}, x_lo)
    tell(barrier, {"gx": gx + 1}, x_hi)
    for axis in ("gy", "gz"):
        for step in (-1, 1):
            tell(barrier, ring(axis, step))
    ll, lh, hl, hh = both(y_lo, z_lo), both(y_lo, z_hi), both(y_hi, z_lo), both(y_hi, z_hi)
    diagonal = {
        "ll": (ll, {"gy": gy - 1, "gz": gz - 1}),
        "lh": (lh, {"gy": gy - 1, "gz": gz + 1}),
        "hl": (hl, {"gy": gy + 1, "gz": gz - 1}),
        "hh": (hh, {"gy": gy + 1, "gz": gz + 1}),
    }
    for cond, peer in diagonal.values():
        tell(barrier, peer, cond)
    greeted = 4
    for cond in (x_lo, x_hi, ll, lh, hl, hh):
        greeted = greeted + cond.astype(jnp.int32)

    def zero(cond, ref):
        @pl.when(cond)
        def _():
            ref[...] = jnp.zeros(ref.shape, F32)

    zero(no(x_lo), field.at[0:2, 2:18])
    zero(no(x_hi), field.at[18:20, 2:18])
    zero(no(y_lo), field.at[2:18, 0:2])
    zero(no(y_hi), field.at[2:18, 18:20])
    zero(no(y_lo), zmid.at[0])
    zero(no(y_hi), zmid.at[9])
    zero(no(z_lo), zlow.at[1:9])
    zero(no(z_hi), zhigh.at[1:9])
    zero(no(ll), zlow.at[0])
    zero(no(lh), zhigh.at[0])
    zero(no(hl), zlow.at[9])
    zero(no(hh), zhigh.at[9])

    lane = lax.broadcasted_iota(jnp.int32, (8, 128), 1)
    sub = lax.broadcasted_iota(jnp.int32, (8, 128), 0)
    slot_of = ((lane + 2) & 127) >> 2
    quarter = lane & 3

    for load in loads:
        load.wait()

    packed = [jnp.zeros((8, 128), F32) for _ in range(8)]
    for s in range(32):
        mine = slot_of == s
        for b in range(8):
            row = field[s // 2 + 2, 2 * b + s % 2 + 2]
            moved = pltpu.roll(row, 4 * s, 1) if s else row
            packed[b] = jnp.where(mine, moved, packed[b])
    for b in range(8):
        zmid[b + 1] = packed[b]

    pl.semaphore_wait(barrier, greeted)

    halos = []

    def halo(sent, src, dst, peer, came):
        i = len(halos)
        copy = pltpu.make_async_remote_copy(
            src_ref=src,
            dst_ref=dst,
            send_sem=halo_send.at[i],
            recv_sem=halo_recv.at[i],
            device_id=peer,
            device_id_type=MESH,
        )
        halos.append((sent, copy, came))

    halo(z_hi, zmid.at[1:9], zlow.at[1:9], {"gz": gz + 1}, z_lo)
    halo(z_lo, zmid.at[1:9], zhigh.at[1:9], {"gz": gz - 1}, z_hi)
    halo(hh, zmid.at[8], zlow.at[0], diagonal["hh"][1], ll)
    halo(hl, zmid.at[8], zhigh.at[0], diagonal["hl"][1], lh)
    halo(lh, zmid.at[1], zlow.at[9], diagonal["lh"][1], hl)
    halo(ll, zmid.at[1], zhigh.at[9], diagonal["ll"][1], hh)
    halo(y_hi, zmid.at[8], zmid.at[0], {"gy": gy + 1}, y_lo)
    halo(y_lo, zmid.at[1], zmid.at[9], {"gy": gy - 1}, y_hi)
    halo(y_hi, field.at[2:18, 16:18], field.at[2:18, 0:2], {"gy": gy + 1}, y_lo)
    halo(y_lo, field.at[2:18, 2:4], field.at[2:18, 18:20], {"gy": gy - 1}, y_hi)
    halo(x_hi, field.at[16:18, 2:18], field.at[0:2, 2:18], {"gx": gx + 1}, x_lo)
    halo(x_lo, field.at[2:4, 2:18], field.at[18:20, 2:18], {"gx": gx - 1}, x_hi)
    for sent, copy, _ in halos:
        when(sent, copy.start)

    for base, axis in ((0, "gy"), (4, "gz")):
        tell(know.at[base], ring(axis, -1))
        tell(know.at[base + 1], ring(axis, 1))
    tell(know.at[8], {"gx": gx - 1}, both(x_lo, x_hi))
    tell(know.at[9], {"gx": gx + 1}, both(x_lo, x_hi))

    def shifts(f):
        return (pltpu.roll(f, k, 1) for k in (127, 126, 1, 2))

    def along_z(i, _):
        for j in range(2):
            x = 2 * i + j
            for y in range(16):
                up1, up2, down1, down2 = shifts(field[x + 2, y + 2])
                firsts[x, y + 2] = 8.0 * (up1 - down1) - (up2 - down2)
                seconds[x, y] = 16.0 * (up1 + down1) - (up2 + down2)
        return 0

    lax.fori_loop(0, 8, along_z, 0)

    for base, axis in ((0, "gy"), (4, "gz")):
        hear(know.at[base])
        hear(know.at[base + 1])
        tell(know.at[base + 2], ring(axis, -2))
        tell(know.at[base + 3], ring(axis, 2))
    hear(know.at[8], gx + 2 < nx)
    hear(know.at[9], gx >= 2)
    tell(know.at[10], {"gx": gx - 2}, both(gx >= 2, x_hi))
    tell(know.at[11], {"gx": gx + 2}, both(gx + 2 < nx, x_lo))

    def arrive(i):
        when(halos[i][2], halos[i][1].wait_recv)

    for i in range(8):
        arrive(i)

    signs = jnp.where(sub < 4, 1.0 / 24.0, -1.0 / 24.0).astype(F32)
    ups, downs, errors = [], [], []
    bends = []
    for b in range(10):
        wrong = jnp.where(quarter >= 2, zlow[b], zhigh[b]) - zmid[b]
        near = jnp.where(
            quarter == 0, pltpu.roll(wrong, 1, 1), jnp.where(quarter == 3, pltpu.roll(wrong, 127, 1), 0.0)
        )
        far = jnp.where(quarter < 2, pltpu.roll(wrong, 2, 1), pltpu.roll(wrong, 126, 1))
        slope = far - 8.0 * near
        slope = jnp.where(quarter < 2, slope, -slope)
        errors.append(slope)
        ups.append(pltpu.roll(slope, 124, 1))
        downs.append(pltpu.roll(slope, 4, 1))
        bends.append(16.0 * near - far)
    even = (slot_of & 1) == 0
    for b in range(1, 9):
        step1 = jnp.where(even, ups[b] - ups[b - 1], downs[b + 1] - downs[b])
        mixed = 8.0 * step1 - (errors[b + 1] - errors[b - 1])
        edge[b - 1] = -(bends[b] * signs) - pltpu.roll(mixed, 4, 0) * (1.0 / 144.0)

    step_of = sub & 3
    at_end = jnp.logical_or(lane < 2, lane >= 126)
    uz = (lane + gz * 128).astype(F32)
    uz = (uz + 0.5) / (nz * 128) - 0.5
    uz2 = uz * uz + 0.05

    def rows(xs, ys, total):
        lefts, rights = [], []
        for x in xs:
            ux = (x + gx * 16).astype(F32)
            ux = (ux + 0.5) / (nx * 16) - 0.5
            ux2 = uz2 + ux * ux
            for y in ys:
                f = field[x + 2, y + 2]
                near = (field[x + 1, y + 2] + field[x + 3, y + 2]) + (field[x + 2, y + 1] + field[x + 2, y + 3])
                far = (field[x, y + 2] + field[x + 4, y + 2]) + (field[x + 2, y] + field[x + 2, y + 4])
                combo = (16.0 * near - far) - (seconds[x, y] + 30.0 * f)
                mixed = 8.0 * (firsts[x, y + 3] - firsts[x, y + 1]) - (firsts[x, y + 4] - firsts[x, y])
                end = pltpu.roll(edge[y // 2], 128 - 4 * (2 * x + y % 2), 1)
                value = combo * signs - pltpu.roll(mixed, 4, 0) * (1.0 / 144.0)
                value = value + jnp.where(at_end, end, 0.0)
                psi_out[x, y] = value
                news = value + jnp.where(step_of >= 1, pltpu.roll(value, 1, 0), 0.0)
                news = news + jnp.where(step_of >= 2, pltpu.roll(news, 2, 0), 0.0)
                power = news * news
                power = power + pltpu.roll(power, 4, 0)
                uy = (gy * 16 + y).astype(F32)
                uy = (uy + 0.5) / (ny * 16) - 0.5
                flux = power * ((ux2 + uy * uy) * 0.0625)
                high = flux.astype(jnp.bfloat16).astype(F32)
                split = jnp.where(sub < 4, high, flux - high)
                label = jnp.broadcast_to(shell[x, pl.ds(y, 1), :], (8, 128))
                outer = label >> 5
                inner = label & 31
                lefts.append(
                    jnp.concatenate([jnp.where(outer == k, split, 0.0) for k in range(8)], axis=0)
                )
                rights.append(
                    jnp.concatenate(
                        [jnp.where(inner == sub + 8 * j, 1.0, 0.0).astype(F32) for j in range(4)], axis=0
                    )
                )
        left = jnp.concatenate(lefts, axis=1)
        right = jnp.concatenate(rights, axis=1)
        return total + lax.dot_general(
            left, right, (((1,), (1,)), ((), ())), preferred_element_type=F32
        )

    total = jnp.zeros((64, 32), F32)
    total = lax.fori_loop(2, 14, lambda x, t: rows([x], range(2, 14), t), total)

    for i in range(8, 12):
        arrive(i)

    def along_z_ends(i, _):
        for j in range(8):
            x = 8 * i + j
            for y in (0, 1, 18, 19):
                up1, up2, down1, down2 = shifts(field[x + 2, y])
                firsts[x, y] = 8.0 * (up1 - down1) - (up2 - down2)
        return 0

    lax.fori_loop(0, 2, along_z_ends, 0)

    total = lax.fori_loop(
        0, 3, lambda i, t: rows([4 * i + 2 + j for j in range(4)], (0, 1, 14, 15), t), total
    )
    total = lax.fori_loop(
        0, 4, lambda i, t: rows([i + 12 * (i // 2)], range(16), t), total
    )

    for base in (0, 4):
        hear(know.at[base + 2])
        hear(know.at[base + 3])
    hear(know.at[10], gx + 3 < nx)
    hear(know.at[11], gx >= 3)
    tell(know.at[12], {"gx": gx - 4}, both(gx >= 4, x_hi))

    def by_step(x, moves):
        moved = x
        for t in range(1, 4):
            moved = jnp.where(step_of == t, pltpu.roll(x, moves[t], 1), moved)
        return moved

    binned[...] = jnp.zeros((64, 128), F32)
    binned[:, 0:32] = total
    for k in range(8):
        spread = by_step(binned[8 * k : 8 * k + 8, :], (0, 32, 64, 96))
        parts[k] = jnp.sum(spread, axis=0, keepdims=True)

    sums = []

    def pass_on(i, sent, src, dst, peer, came):
        copy = pltpu.make_async_remote_copy(
            src_ref=src,
            dst_ref=dst,
            send_sem=sum_send.at[i],
            recv_sem=sum_recv.at[i],
            device_id=peer,
            device_id_type=MESH,
        )
        sums.append((sent, copy))
        when(sent, copy.start)
        return lambda: when(came, copy.wait_recv)

    waits = []
    for d in range(1, ny):
        peer = ring("gy", d)
        waits.append(pass_on(d, None, parts.at[peer["gy"]], got_y.at[d], peer, None))
    for wait in waits:
        wait()
    value = parts[gy]
    for d in range(1, ny):
        value = value + got_y[d]

    summed[0] = value
    waits = [pass_on(8 + d, None, summed.at[0], got_z.at[d], ring("gz", d), None) for d in range(1, nz)]
    for wait in waits:
        wait()
    for d in range(1, nz):
        value = value + got_z[d]

    summed[1] = value
    hear(know.at[12], gx + 5 < nx)
    waits = [
        pass_on(16 + d, gx + d < nx, summed.at[1], got_x.at[d], {"gx": gx + d}, gx >= d)
        for d in range(1, nx)
    ]
    for wait in waits:
        wait()
    for d in range(1, nx):
        value = value + jnp.where(gx >= d, got_x[d], 0.0)

    first = jnp.broadcast_to(onsets[pl.ds(gy // 4, 1), :], (8, 128))
    first = pltpu.roll(first, lax.rem(128 - 32 * lax.rem(gy, 4), 128), 1)
    first = jnp.where(lane < 32, first, 0)
    first = first + pltpu.roll(first, 32, 1)
    first = first + pltpu.roll(first, 64, 1)
    value = jnp.broadcast_to(value, (8, 128))
    value = jnp.where((lane >> 5) >= first, value, 0.0)
    value = value + jnp.where(lane >= 32, pltpu.roll(value, 32, 1), 0.0)
    value = value + jnp.where(lane >= 64, pltpu.roll(value, 64, 1), 0.0)
    value = value * (0.25 * 256 / (nx * 16 * ny * 16 * nz * 128))
    value = pltpu.roll(value, lax.rem(128 - 4 * gz, 128), 1)
    value = by_step(value, (0, 96, 64, 32))
    energy_out[0] = value[0:4, 0:4]

    for sent, copy, _ in halos:
        when(sent, copy.wait_send)
    for sent, copy in sums:
        when(sent, copy.wait_send)


def write(psi, energy, psi_out, energy_out, sem):
    copies = [pltpu.make_async_copy(psi.at[:, :, c], psi_out.at[c], sem.at[c]) for c in range(CT)]
    copies.append(pltpu.make_async_copy(energy, energy_out, sem.at[CT]))
    for copy in copies:
        copy.start()
    for copy in copies:
        copy.wait()


def solution(mesh):
    sizes = tuple(mesh.shape[a] for a in ("gx", "gy", "gz"))
    vmem = pl.BlockSpec(memory_space=pltpu.VMEM)
    hbm = pl.BlockSpec(memory_space=pltpu.HBM)

    def body(strain, cell_shell_index, onset_step):
        psi, energy = pl.pallas_call(
            lambda *refs: kernel(sizes, *refs),
            out_shape=(pltpu.VMEM((16, 16, 8, 128), F32), pltpu.VMEM((1, 4, 4), F32)),
            in_specs=[hbm] * 3,
            out_specs=(vmem, vmem),
            scratch_shapes=[
                pltpu.VMEM((20, 20, 8, 128), F32),
                pltpu.VMEM((16, 16, 128), jnp.int32),
                pltpu.VMEM((2, 128), jnp.int32),
                pltpu.VMEM((10, 8, 128), F32),
                pltpu.VMEM((10, 8, 128), F32),
                pltpu.VMEM((10, 8, 128), F32),
                pltpu.VMEM((8, 8, 128), F32),
                pltpu.VMEM((16, 20, 8, 128), F32),
                pltpu.VMEM((16, 16, 8, 128), F32),
                pltpu.VMEM((64, 128), F32),
                pltpu.VMEM((8, 1, 128), F32),
                pltpu.VMEM((8, 1, 128), F32),
                pltpu.VMEM((8, 1, 128), F32),
                pltpu.VMEM((8, 1, 128), F32),
                pltpu.VMEM((2, 1, 128), F32),
                pltpu.SemaphoreType.DMA((10,)),
                pltpu.SemaphoreType.DMA((12,)),
                pltpu.SemaphoreType.DMA((12,)),
                pltpu.SemaphoreType.DMA((24,)),
                pltpu.SemaphoreType.DMA((24,)),
                pltpu.SemaphoreType.REGULAR((13,)),
            ],
            compiler_params=pltpu.CompilerParams(collective_id=0, has_side_effects=True),
        )(strain.reshape(8, 16, 16, 128), cell_shell_index, onset_step.reshape(2, 128))
        psi_four, energy = pl.pallas_call(
            write,
            out_shape=(
                jax.ShapeDtypeStruct((8, 16, 16, 128), F32),
                jax.ShapeDtypeStruct((1, 4, 4), F32),
            ),
            in_specs=[vmem] * 2,
            out_specs=(hbm, hbm),
            scratch_shapes=[pltpu.SemaphoreType.DMA((CT + 1,))],
        )(*(pltpu.with_memory_space_constraint(a, pltpu.VMEM) for a in (psi, energy)))
        return psi_four.reshape(strain.shape), energy

    placed = (P(None, None, "gx", "gy", "gz"), P("gx", "gy", "gz"), P())
    return jax.shard_map(
        body,
        mesh=mesh,
        in_specs=placed,
        out_specs=(P(None, None, "gx", "gy", "gz"), P("gx", None, ("gy", "gz"))),
        check_vma=False,
    )
```

```python
import jax
import jax.numpy as jnp
from jax import lax
from jax.experimental import pallas as pl
from jax.experimental.pallas import tpu as pltpu
from jax.sharding import PartitionSpec as P

MESH = pl.DeviceIdType.MESH
F32 = jnp.float32
CT = 8


def kernel(
    sizes,
    strain,
    shells,
    onset,
    psi_out,
    energy_out,
    field,
    shell,
    onsets,
    zmid,
    zlow,
    zhigh,
    outer,
    inner,
    firsts,
    seconds,
    binned,
    parts,
    got,
    got_x,
    summed,
    in_sem,
    sent_sem,
    came_sem,
    know,
):
    nx, ny, nz = sizes
    gx, gy, gz = (lax.axis_index(a) for a in ("gx", "gy", "gz"))
    no = jnp.logical_not
    both = jnp.logical_and

    for h in range(2):
        for c in range(CT):
            pltpu.make_async_copy(
                strain.at[c, 8 * h : 8 * h + 8],
                field.at[8 * h + 2 : 8 * h + 10, 2:18, c],
                in_sem.at[h],
            ).start()
    labels = pltpu.make_async_copy(shells, shell, in_sem.at[2])
    starts = pltpu.make_async_copy(onset, onsets, in_sem.at[3])
    labels.start()
    starts.start()

    def when(cond, act):
        if cond is None:
            act()
        else:
            pl.when(cond)(act)

    def tell(sem, peer, cond=None):
        when(cond, lambda: pl.semaphore_signal(sem, inc=1, device_id=peer, device_id_type=MESH))

    def total_of(conds):
        return sum(c.astype(jnp.int32) for c in conds)

    def near_to(dy, dz):
        peer = {}
        if dy:
            peer["gy"] = lax.rem(gy + (dy + ny), ny)
        if dz:
            peer["gz"] = lax.rem(gz + (dz + nz), nz)
        return peer

    around = [(dy, dz) for dy in (-1, 0, 1) for dz in (-1, 0, 1) if dy or dz]

    barrier = pltpu.get_barrier_semaphore()
    x_lo, x_hi = gx > 0, gx < nx - 1
    y_lo, y_hi = gy > 0, gy < ny - 1
    z_lo, z_hi = gz > 0, gz < nz - 1
    half = nx // 2
    late = both(x_hi, gx < half)
    tell(barrier, {"gx": gx - 1}, gx > half)
    for step in around:
        tell(barrier, near_to(*step))
    for d in range(1, nx):
        tell(barrier, {"gx": gx + d}, gx + d < nx)
    greeted = 8 + gx + total_of((both(x_hi, gx >= half),))

    def zero(cond, ref):
        @pl.when(cond)
        def _():
            ref[...] = jnp.zeros(ref.shape, F32)

    zero(no(x_lo), field.at[0:2, 2:18])
    zero(no(x_hi), field.at[18:20, 2:18])

    lane = lax.broadcasted_iota(jnp.int32, (8, 128), 1)
    sub = lax.broadcasted_iota(jnp.int32, (8, 128), 0)
    slot_of = ((lane + 2) & 127) >> 2
    quarter = lane & 3

    packed = [jnp.zeros((8, 128), F32) for _ in range(8)]
    for s in range(32):
        if s % 16 == 0:
            own = field.at[s // 2 + 2 : s // 2 + 10, 2:18]
            pltpu.make_async_copy(own, own, in_sem.at[s // 16]).wait()
        mine = slot_of == s
        for b in range(8):
            row = field[s // 2 + 2, 2 * b + s % 2 + 2]
            moved = pltpu.roll(row, 4 * s, 1) if s else row
            packed[b] = jnp.where(mine, moved, packed[b])
    for b in range(8):
        zmid[b + 1] = packed[b]

    pl.semaphore_wait(barrier, greeted)

    def remote(src, dst, send, recv, peer):
        return pltpu.make_async_remote_copy(
            src_ref=src, dst_ref=dst, send_sem=send, recv_sem=recv, device_id=peer, device_id_type=MESH
        )

    z_halos = [
        (zmid.at[1:9], zlow.at[1:9], (0, 1)),
        (zmid.at[1:9], zhigh.at[1:9], (0, -1)),
        (zmid.at[8], zlow.at[0], (1, 1)),
        (zmid.at[8], zhigh.at[0], (1, -1)),
        (zmid.at[1], zlow.at[9], (-1, 1)),
        (zmid.at[1], zhigh.at[9], (-1, -1)),
        (zmid.at[8], zmid.at[0], (1, 0)),
        (zmid.at[1], zmid.at[9], (-1, 0)),
    ]
    y_halos = [
        (field.at[2:18, 16:18], field.at[2:18, 0:2], (1, 0)),
        (field.at[2:18, 2:4], field.at[2:18, 18:20], (-1, 0)),
    ]
    for i, group in enumerate((z_halos, y_halos)):
        for src, dst, step in group:
            remote(src, dst, sent_sem.at[i], came_sem.at[i], near_to(*step)).start()
    x_down = remote(
        field.at[2:4, 2:18], field.at[18:20, 2:18], sent_sem.at[2], came_sem.at[2], {"gx": gx - 1}
    )
    x_up = remote(
        field.at[16:18, 2:18], field.at[0:2, 2:18], sent_sem.at[3], came_sem.at[3], {"gx": gx + 1}
    )
    when(x_lo, x_down.start)
    when(both(x_hi, gx >= half), x_up.start)

    tell(know.at[0], {"gx": gx - 1}, both(x_lo, gx <= half))
    for step in around:
        tell(know.at[1], near_to(*step))
    for d in range(1, nx):
        tell(know.at[3], {"gx": gx - d}, gx >= d)

    labels.wait()
    starts.wait()
    outer[...] = shell[...] >> 5
    inner[...] = shell[...] & 31
    first = jnp.broadcast_to(onsets[pl.ds(gy // 4, 1), :], (8, 128))
    first = pltpu.roll(first, lax.rem(128 - 32 * lax.rem(gy, 4), 128), 1)
    first = jnp.where(lane < 32, first, 0)
    first = first + pltpu.roll(first, 32, 1)
    first = first + pltpu.roll(first, 64, 1)

    signs = jnp.where(sub < 4, 1.0 / 24.0, -1.0 / 24.0).astype(F32)
    minus = -signs

    def shifts(f):
        return (pltpu.roll(f, k, 1) for k in (127, 126, 1, 2))

    def slope(up1, up2, down1, down2):
        d = (up1 - down1) * (8.0 / 144.0) - (up2 - down2) * (1.0 / 144.0)
        return pltpu.roll(d, 4, 0)

    def along_z(i, _):
        for j in range(2):
            x = 2 * i + j
            for y in range(16):
                f = field[x + 2, y + 2]
                up1, up2, down1, down2 = shifts(f)
                firsts[x, y + 2] = slope(up1, up2, down1, down2)
                bend = 16.0 * (up1 + down1) - (up2 + down2)
                seconds[x, y] = (bend + 30.0 * f) * minus
        return 0

    lax.fori_loop(0, 8, along_z, 0)

    pl.semaphore_wait(know.at[1], 8)
    for dy, dz in around:
        tell(know.at[2], near_to(2 * dy, 2 * dz))

    when(late, lambda: pl.semaphore_wait(know.at[0], 1))
    when(late, x_up.start)

    def arrive(i, ref):
        pltpu.make_async_copy(ref, ref, came_sem.at[i]).wait()

    arrive(0, field.at[0:2, 0:11])

    ups, downs, errors = [], [], []
    bends = []
    for b in range(10):
        low, high, mid = zlow[b], zhigh[b], zmid[b]
        in_y = {0: y_lo, 9: y_hi}.get(b)
        has_low, has_high = z_lo, z_hi
        if in_y is not None:
            has_low, has_high = both(z_lo, in_y), both(z_hi, in_y)
            mid = jnp.where(in_y, mid, 0.0)
        low, high = jnp.where(has_low, low, 0.0), jnp.where(has_high, high, 0.0)
        wrong = jnp.where(quarter >= 2, low, high) - mid
        near = jnp.where(
            quarter == 0, pltpu.roll(wrong, 1, 1), jnp.where(quarter == 3, pltpu.roll(wrong, 127, 1), 0.0)
        )
        far = jnp.where(quarter < 2, pltpu.roll(wrong, 2, 1), pltpu.roll(wrong, 126, 1))
        error = far - 8.0 * near
        error = jnp.where(quarter < 2, error, -error)
        errors.append(error)
        ups.append(pltpu.roll(error, 124, 1))
        downs.append(pltpu.roll(error, 4, 1))
        bends.append(16.0 * near - far)
    even = (slot_of & 1) == 0
    at_end = jnp.logical_or(lane < 2, lane >= 126)
    for b in range(1, 9):
        step1 = jnp.where(even, ups[b] - ups[b - 1], downs[b + 1] - downs[b])
        mixed = 8.0 * step1 - (errors[b + 1] - errors[b - 1])
        fix = bends[b] * minus - pltpu.roll(mixed, 4, 0) * (1.0 / 144.0)
        for s in range(32):
            x, y = s // 2, 2 * b - 2 + s % 2
            end = pltpu.roll(fix, 128 - 4 * s, 1) if s else fix
            seconds[x, y] = seconds[x, y] + jnp.where(at_end, end, 0.0)

    step_of = sub & 3
    uz = (lane + gz * 128).astype(F32)
    uz = (uz + 0.5) / (nz * 128) - 0.5
    uz2 = (uz * uz + 0.05) * 0.0625

    def rows(xs, ys, total):
        lefts, rights = [], []
        for x in xs:
            ux = (x + gx * 16).astype(F32)
            ux = (ux + 0.5) / (nx * 16) - 0.5
            ux2 = uz2 + ux * ux * 0.0625
            for y in ys:
                near = (field[x + 1, y + 2] + field[x + 3, y + 2]) + (field[x + 2, y + 1] + field[x + 2, y + 3])
                far = (field[x, y + 2] + field[x + 4, y + 2]) + (field[x + 2, y] + field[x + 2, y + 4])
                mixed = 8.0 * (firsts[x, y + 3] - firsts[x, y + 1]) - (firsts[x, y + 4] - firsts[x, y])
                value = (16.0 * near - far) * signs + (seconds[x, y] - mixed)
                psi_out[x, y] = value
                news = value + jnp.where(step_of >= 1, pltpu.roll(value, 1, 0), 0.0)
                news = news + jnp.where(step_of >= 2, pltpu.roll(news, 2, 0), 0.0)
                power = news * news
                power = power + pltpu.roll(power, 4, 0)
                uy = (gy * 16 + y).astype(F32)
                uy = (uy + 0.5) / (ny * 16) - 0.5
                flux = power * (ux2 + uy * uy * 0.0625)
                high = flux.astype(jnp.bfloat16).astype(F32)
                split = jnp.where(sub < 4, high, flux - high)
                high_label = jnp.broadcast_to(outer[x, pl.ds(y, 1), :], (8, 128))
                low_label = jnp.broadcast_to(inner[x, pl.ds(y, 1), :], (8, 128))
                lefts.append(
                    jnp.concatenate([jnp.where(high_label == k, split, 0.0) for k in range(8)], axis=0)
                )
                rights.append(
                    jnp.concatenate(
                        [jnp.where(low_label == sub + 8 * j, 1.0, 0.0).astype(F32) for j in range(4)], axis=0
                    )
                )
        left = jnp.concatenate(lefts, axis=1)
        right = jnp.concatenate(rights, axis=1)
        return total + lax.dot_general(
            left, right, (((1,), (1,)), ((), ())), preferred_element_type=F32
        )

    total = jnp.zeros((64, 32), F32)
    total = lax.fori_loop(0, 4, lambda i, t: rows([3 * i + 2 + j for j in range(3)], range(2, 14), t), total)

    arrive(1, field.at[0:16, 0:4])
    when(x_hi, x_down.wait_recv)
    when(x_lo, x_up.wait_recv)
    zero(no(y_lo), field.at[2:18, 0:2])
    zero(no(y_hi), field.at[2:18, 18:20])

    def along_z_ends(i, _):
        for j in range(8):
            x = 8 * i + j
            for y in (0, 1, 18, 19):
                up1, up2, down1, down2 = shifts(field[x + 2, y])
                firsts[x, y] = slope(up1, up2, down1, down2)
        return 0

    lax.fori_loop(0, 2, along_z_ends, 0)

    total = rows(range(2, 14), (0, 1, 14, 15), total)
    total = lax.fori_loop(
        0, 2, lambda i, t: rows([14 * i, 14 * i + 1], range(16), t), total
    )

    pl.semaphore_wait(know.at[2], 8)

    def by_step(x, moves):
        moved = x
        for t in range(1, 4):
            moved = jnp.where(step_of == t, pltpu.roll(x, moves[t], 1), moved)
        return moved

    binned[...] = jnp.zeros((64, 128), F32)
    binned[:, 0:32] = total
    for k in range(8):
        spread = by_step(binned[8 * k : 8 * k + 8, :], (0, 32, 64, 96))
        parts[k] = jnp.sum(spread, axis=0, keepdims=True)

    offsets = [(dy, dz) for dy in range(ny) for dz in range(nz) if dy or dz]
    offsets.sort(key=lambda o: -(min(o[0], ny - o[0]) + min(o[1], nz - o[1]) / 2))
    for i, (dy, dz) in enumerate(offsets):
        peer = near_to(dy, dz)
        remote(parts.at[peer.get("gy", gy)], got.at[i], sent_sem.at[4], came_sem.at[4], peer).start()

    arrive(4, got)
    sums = [parts[gy]] + [got[i] for i in range(len(offsets))]
    while len(sums) > 1:
        sums = [a + b for a, b in zip(sums[::2], sums[1::2])]
    value = sums[0]

    summed[0] = value
    when(x_hi, lambda: pl.semaphore_wait(know.at[3], nx - 1 - gx))
    for d in range(1, nx):
        copy = remote(summed.at[0], got_x.at[d - 1], sent_sem.at[5], came_sem.at[5], {"gx": gx + d})
        when(gx + d < nx, copy.start)
    for n in range(1, nx):
        when(gx == n, lambda n=n: arrive(5, got_x.at[0:n]))
    for d in range(1, nx):
        value = value + jnp.where(gx >= d, got_x[d - 1], 0.0)

    value = jnp.broadcast_to(value, (8, 128))
    value = jnp.where((lane >> 5) >= first, value, 0.0)
    value = value * (0.25 * 256 / (nx * 16 * ny * 16 * nz * 128))
    steps = [pltpu.roll(value, lax.rem(256 - 32 * t - 4 * gz, 128), 1) for t in range(4)]
    value = steps[0]
    for t in range(1, 4):
        value = value + jnp.where(sub >= t, steps[t], 0.0)
    energy_out[0] = value[0:4, 0:4]

    def left(i, ref):
        pltpu.make_async_copy(ref, ref, sent_sem.at[i]).wait()

    left(0, field.at[0:2, 0:11])
    left(1, field.at[0:16, 0:4])
    when(x_lo, x_down.wait_send)
    when(x_hi, x_up.wait_send)
    left(4, got)
    for n in range(1, nx):
        when(gx == nx - 1 - n, lambda n=n: left(5, got_x.at[0:n]))


def write(psi, energy, psi_out, energy_out, sem):
    for c in range(CT):
        pltpu.make_async_copy(psi.at[:, :, c], psi_out.at[c], sem.at[0]).start()
    small = pltpu.make_async_copy(energy, energy_out, sem.at[1])
    small.start()
    pltpu.make_async_copy(psi_out, psi_out, sem.at[0]).wait()
    small.wait()


def solution(mesh):
    sizes = tuple(mesh.shape[a] for a in ("gx", "gy", "gz"))
    vmem = pl.BlockSpec(memory_space=pltpu.VMEM)
    hbm = pl.BlockSpec(memory_space=pltpu.HBM)

    def body(strain, cell_shell_index, onset_step):
        psi, energy = pl.pallas_call(
            lambda *refs: kernel(sizes, *refs),
            out_shape=(pltpu.VMEM((16, 16, 8, 128), F32), pltpu.VMEM((1, 4, 4), F32)),
            in_specs=[hbm] * 3,
            out_specs=(vmem, vmem),
            scratch_shapes=[
                pltpu.VMEM((20, 20, 8, 128), F32),
                pltpu.VMEM((16, 16, 128), jnp.int32),
                pltpu.VMEM((2, 128), jnp.int32),
                pltpu.VMEM((10, 8, 128), F32),
                pltpu.VMEM((10, 8, 128), F32),
                pltpu.VMEM((10, 8, 128), F32),
                pltpu.VMEM((16, 16, 128), jnp.int32),
                pltpu.VMEM((16, 16, 128), jnp.int32),
                pltpu.VMEM((16, 20, 8, 128), F32),
                pltpu.VMEM((16, 16, 8, 128), F32),
                pltpu.VMEM((64, 128), F32),
                pltpu.VMEM((8, 1, 128), F32),
                pltpu.VMEM((63, 1, 128), F32),
                pltpu.VMEM((7, 1, 128), F32),
                pltpu.VMEM((1, 1, 128), F32),
                pltpu.SemaphoreType.DMA((4,)),
                pltpu.SemaphoreType.DMA((6,)),
                pltpu.SemaphoreType.DMA((6,)),
                pltpu.SemaphoreType.REGULAR((4,)),
            ],
            compiler_params=pltpu.CompilerParams(collective_id=0, has_side_effects=True),
        )(strain.reshape(8, 16, 16, 128), cell_shell_index, onset_step.reshape(2, 128))
        psi_four, energy = pl.pallas_call(
            write,
            out_shape=(
                jax.ShapeDtypeStruct((8, 16, 16, 128), F32),
                jax.ShapeDtypeStruct((1, 4, 4), F32),
            ),
            in_specs=[vmem] * 2,
            out_specs=(hbm, hbm),
            scratch_shapes=[pltpu.SemaphoreType.DMA((2,))],
        )(*(pltpu.with_memory_space_constraint(a, pltpu.VMEM) for a in (psi, energy)))
        return psi_four.reshape(strain.shape), energy

    placed = (P(None, None, "gx", "gy", "gz"), P("gx", "gy", "gz"), P())
    return jax.shard_map(
        body,
        mesh=mesh,
        in_specs=placed,
        out_specs=(P(None, None, "gx", "gy", "gz"), P("gx", None, ("gy", "gz"))),
        check_vma=False,
    )
```

```python
import jax
import jax.numpy as jnp
from jax import lax
from jax.experimental import pallas as pl
from jax.experimental.pallas import tpu as pltpu
from jax.sharding import PartitionSpec as P

MESH = pl.DeviceIdType.MESH
F32 = jnp.float32
CT = 8


def kernel(
    sizes,
    strain,
    shells,
    onset,
    psi_out,
    energy_out,
    field,
    shell,
    onsets,
    zmid,
    zlow,
    zhigh,
    outer,
    inner,
    firsts,
    seconds,
    binned,
    parts,
    got,
    got_x,
    summed,
    in_sem,
    sent_sem,
    came_sem,
    know,
):
    nx, ny, nz = sizes
    gx, gy, gz = (lax.axis_index(a) for a in ("gx", "gy", "gz"))
    no = jnp.logical_not
    both = jnp.logical_and

    def when(cond, act):
        if cond is None:
            act()
        else:
            pl.when(cond)(act)

    def tell(sem, peer, cond=None):
        when(cond, lambda: pl.semaphore_signal(sem, inc=1, device_id=peer, device_id_type=MESH))

    def total_of(conds):
        return sum(c.astype(jnp.int32) for c in conds)

    def near_to(dy, dz):
        peer = {}
        if dy:
            peer["gy"] = lax.rem(gy + (dy + ny), ny)
        if dz:
            peer["gz"] = lax.rem(gz + (dz + nz), nz)
        return peer

    around = [(dy, dz) for dy in (-1, 0, 1) for dz in (-1, 0, 1) if dy or dz]

    barrier = pltpu.get_barrier_semaphore()
    x_lo, x_hi = gx > 0, gx < nx - 1
    y_lo, y_hi = gy > 0, gy < ny - 1
    z_lo, z_hi = gz > 0, gz < nz - 1
    half = nx // 2
    late, soon = both(x_hi, gx < half), both(x_hi, gx >= half)
    for step in around:
        tell(barrier, near_to(*step))
    for d in range(1, nx):
        tell(barrier, {"gx": gx + d}, gx + d < nx)
    greeted = 8 + gx

    for h in range(2):
        for c in range(CT):
            pltpu.make_async_copy(
                strain.at[c, 8 * h : 8 * h + 8],
                field.at[8 * h + 2 : 8 * h + 10, 2:18, c],
                in_sem.at[h],
            ).start()
    labels = pltpu.make_async_copy(shells, shell, in_sem.at[2])
    starts = pltpu.make_async_copy(onset, onsets, in_sem.at[3])
    labels.start()
    starts.start()

    def zero(cond, ref):
        @pl.when(cond)
        def _():
            ref[...] = jnp.zeros(ref.shape, F32)

    zero(no(x_lo), field.at[0:2, 2:18])
    zero(no(x_hi), field.at[18:20, 2:18])
    zero(no(y_lo), field.at[2:18, 0:2])
    zero(no(y_hi), field.at[2:18, 18:20])
    zero(no(y_lo), zmid.at[0])
    zero(no(y_hi), zmid.at[9])
    zero(no(z_lo), zlow.at[1:9])
    zero(no(z_hi), zhigh.at[1:9])
    zero(no(both(y_lo, z_lo)), zlow.at[0])
    zero(no(both(y_hi, z_lo)), zlow.at[9])
    zero(no(both(y_lo, z_hi)), zhigh.at[0])
    zero(no(both(y_hi, z_hi)), zhigh.at[9])

    lane = lax.broadcasted_iota(jnp.int32, (8, 128), 1)
    sub = lax.broadcasted_iota(jnp.int32, (8, 128), 0)
    slot_of = ((lane + 2) & 127) >> 2
    quarter = lane & 3

    for h in range(2):
        own = field.at[8 * h + 2 : 8 * h + 10, 2:18]
        pltpu.make_async_copy(own, own, in_sem.at[h]).wait()

    packed = [jnp.zeros((8, 128), F32) for _ in range(8)]
    for s in range(32):
        mine = slot_of == s
        for b in range(8):
            row = field[s // 2 + 2, 2 * b + s % 2 + 2]
            moved = pltpu.roll(row, 4 * s, 1) if s else row
            packed[b] = jnp.where(mine, moved, packed[b])
    for b in range(8):
        zmid[b + 1] = packed[b]

    pl.semaphore_wait(barrier, greeted)

    tell(know.at[0], {"gx": gx - 1}, x_lo)
    for step in around:
        tell(know.at[1], near_to(*step))
    for d in range(1, nx):
        tell(know.at[3], {"gx": gx - d}, gx >= d)

    def remote(src, dst, send, recv, peer):
        return pltpu.make_async_remote_copy(
            src_ref=src, dst_ref=dst, send_sem=send, recv_sem=recv, device_id=peer, device_id_type=MESH
        )

    halos = [
        (zmid.at[1:9], zlow.at[1:9], (0, 1), 0),
        (zmid.at[1:9], zhigh.at[1:9], (0, -1), 0),
        (zmid.at[8], zlow.at[0], (1, 1), 1),
        (zmid.at[8], zhigh.at[0], (1, -1), 1),
        (zmid.at[1], zlow.at[9], (-1, 1), 1),
        (zmid.at[1], zhigh.at[9], (-1, -1), 1),
        (zmid.at[8], zmid.at[0], (1, 0), 1),
        (zmid.at[1], zmid.at[9], (-1, 0), 1),
    ]
    def send(halos):
        for src, dst, (dy, dz), i in halos:
            is_there = {(0, 1): z_hi, (0, -1): z_lo, (1, 0): y_hi, (-1, 0): y_lo}
            there = is_there.get((dy, dz))
            if there is None:
                there = both(is_there[dy, 0], is_there[0, dz])
            when(there, remote(src, dst, sent_sem.at[i // 2], came_sem.at[i], near_to(dy, dz)).start)
    y_halos = [
        (field.at[2:18, 16:18], field.at[2:18, 0:2], (1, 0), 2),
        (field.at[2:18, 2:4], field.at[2:18, 18:20], (-1, 0), 2),
    ]
    send(halos)
    send(y_halos)
    y_two, z_two = both(y_lo, y_hi), both(z_lo, z_hi)

    def flush(sem, tiles):
        for y_count in (1, 2):
            for z_count in (1, 2):
                n = tiles(y_count, z_count)
                ref = field.at[0, 0:n] if n <= 20 else field.at[0:4, 0 : n // 4] if n % 4 == 0 else field.at[0:2, 0 : n // 2]
                wait = pltpu.make_async_copy(ref, ref, sem).wait
                when(both(y_two if y_count == 2 else no(y_two), z_two if z_count == 2 else no(z_two)), wait)

    x_down = remote(
        field.at[2:4, 2:18], field.at[18:20, 2:18], sent_sem.at[2], came_sem.at[4], {"gx": gx - 1}
    )
    x_up = remote(
        field.at[16:18, 2:18], field.at[0:2, 2:18], sent_sem.at[3], came_sem.at[5], {"gx": gx + 1}
    )
    when(x_lo, x_down.start)

    labels.wait()
    starts.wait()
    outer[...] = shell[...] >> 5
    inner[...] = shell[...] & 31
    first = jnp.broadcast_to(onsets[pl.ds(gy // 4, 1), :], (8, 128))
    first = pltpu.roll(first, lax.rem(128 - 32 * lax.rem(gy, 4), 128), 1)
    first = jnp.where(lane < 32, first, 0)
    first = first + pltpu.roll(first, 32, 1)
    first = first + pltpu.roll(first, 64, 1)

    signs = jnp.where(sub < 4, 1.0 / 24.0, -1.0 / 24.0).astype(F32)
    minus = -signs

    def shifts(f):
        return (pltpu.roll(f, k, 1) for k in (127, 126, 1, 2))

    def slope(up1, up2, down1, down2):
        d = (up1 - down1) * (8.0 / 144.0) - (up2 - down2) * (1.0 / 144.0)
        return pltpu.roll(d, 4, 0)

    def stars(x, y):
        near = (field[x + 1, y + 2] + field[x + 3, y + 2]) + (field[x + 2, y + 1] + field[x + 2, y + 3])
        far = (field[x, y + 2] + field[x + 4, y + 2]) + (field[x + 2, y] + field[x + 2, y + 4])
        return (16.0 * near - far) * signs

    def along_z(xs, whole):
        for x in xs:
            for y in range(16):
                f = field[x + 2, y + 2]
                up1, up2, down1, down2 = shifts(f)
                firsts[x, y + 2] = slope(up1, up2, down1, down2)
                bend = 16.0 * (up1 + down1) - (up2 + down2)
                value = (bend + 30.0 * f) * minus
                if whole and 2 <= y < 14:
                    value = value + stars(x, y)
                seconds[x, y] = value
        return 0

    lax.fori_loop(0, 3, lambda i, _: along_z([4 * i + 2 + j for j in range(4)], True), 0)
    when(soon, lambda: pl.semaphore_wait(know.at[0], 1))
    when(soon, x_up.start)
    lax.fori_loop(0, 2, lambda i, _: along_z([14 * i, 14 * i + 1], False), 0)

    flush(came_sem.at[0], lambda y, z: 8 * z)

    pl.semaphore_wait(know.at[1], 8)
    for dy, dz in around:
        tell(know.at[2], near_to(2 * dy, 2 * dz))

    when(late, lambda: pl.semaphore_wait(know.at[0], 1))
    when(late, x_up.start)

    even = (slot_of & 1) == 0
    at_end = jnp.logical_or(lane < 2, lane >= 126)
    turns = {}

    def turn(b):
        wrong = jnp.where(quarter >= 2, zlow[b], zhigh[b]) - zmid[b]
        near = jnp.where(
            quarter == 0, pltpu.roll(wrong, 1, 1), jnp.where(quarter == 3, pltpu.roll(wrong, 127, 1), 0.0)
        )
        far = jnp.where(quarter < 2, pltpu.roll(wrong, 2, 1), pltpu.roll(wrong, 126, 1))
        error = far - 8.0 * near
        error = jnp.where(quarter < 2, error, -error)
        turns[b] = (error, pltpu.roll(error, 124, 1), pltpu.roll(error, 4, 1), 16.0 * near - far)

    def mend(b):
        (before, before_up, _, _), (_, up, down, bend), (after, _, after_down, _) = (
            turns[b - 1],
            turns[b],
            turns[b + 1],
        )
        step1 = jnp.where(even, up - before_up, after_down - down)
        mixed = 8.0 * step1 - (after - before)
        fix = bend * minus - pltpu.roll(mixed, 4, 0) * (1.0 / 144.0)
        for s in range(32):
            x, y = s // 2, 2 * b - 2 + s % 2
            end = pltpu.roll(fix, 128 - 4 * s, 1) if s else fix
            seconds[x, y] = seconds[x, y] + jnp.where(at_end, end, 0.0)

    for b in range(1, 9):
        turn(b)
    for b in range(2, 8):
        mend(b)

    step_of = sub & 3
    uz = (lane + gz * 128).astype(F32)
    uz = (uz + 0.5) / (nz * 128) - 0.5
    uz2 = (uz * uz + 0.05) * 0.0625

    def rows(xs, ys, whole=False):
        lefts, rights = [], []
        for x in xs:
            ux = (x + gx * 16).astype(F32)
            ux = (ux + 0.5) / (nx * 16) - 0.5
            ux2 = uz2 + ux * ux * 0.0625
            for y in ys:
                mixed = 8.0 * (firsts[x, y + 3] - firsts[x, y + 1]) - (firsts[x, y + 4] - firsts[x, y])
                value = seconds[x, y] - mixed
                if not whole:
                    value = value + stars(x, y)
                psi_out[x, y] = value
                news = value + jnp.where(step_of >= 1, pltpu.roll(value, 1, 0), 0.0)
                news = news + jnp.where(step_of >= 2, pltpu.roll(news, 2, 0), 0.0)
                power = news * news
                power = power + pltpu.roll(power, 4, 0)
                uy = (gy * 16 + y).astype(F32)
                uy = (uy + 0.5) / (ny * 16) - 0.5
                flux = power * (ux2 + uy * uy * 0.0625)
                high = flux.astype(jnp.bfloat16).astype(F32)
                split = jnp.where(sub < 4, high, flux - high)
                high_label = jnp.broadcast_to(outer[x, pl.ds(y, 1), :], (8, 128))
                low_label = jnp.broadcast_to(inner[x, pl.ds(y, 1), :], (8, 128))
                lefts.append(
                    jnp.concatenate([jnp.where(high_label == k, split, 0.0) for k in range(8)], axis=0)
                )
                rights.append(
                    jnp.concatenate(
                        [jnp.where(low_label == sub + 8 * j, 1.0, 0.0).astype(F32) for j in range(4)], axis=0
                    )
                )
        left = jnp.concatenate(lefts, axis=1)
        right = jnp.concatenate(rights, axis=1)
        return lax.dot_general(left, right, (((1,), (1,)), ((), ())), preferred_element_type=F32)

    total = lax.fori_loop(
        0,
        4,
        lambda i, t: t + rows([3 * i + 2 + j for j in range(3)], range(2, 14), True),
        jnp.zeros((64, 32), F32),
    )
    binned[...] = jnp.zeros((64, 128), F32)
    binned[:, 0:32] = total

    def x_rows():
        when(x_hi, x_down.wait_recv)
        when(x_lo, x_up.wait_recv)
        binned[:, 0:32] += rows((0, 1, 14, 15), range(2, 14))

    x_last = jnp.logical_or(gx == half - 1, gx == half)

    def y_rows():
        flush(came_sem.at[1], lambda y, z: y * (z + 1))
        flush(came_sem.at[2], lambda y, z: 32 * y)

        def y_ends(xs):
            for x in xs:
                for y in (0, 1, 18, 19):
                    up1, up2, down1, down2 = shifts(field[x + 2, y])
                    firsts[x, y] = slope(up1, up2, down1, down2)

        y_ends(range(16))
        for b in (0, 1, 2, 7, 8, 9):
            turn(b)
        for b in (1, 8):
            mend(b)
        binned[:, 0:32] += rows(range(2, 14), (0, 1, 14, 15))

    def in_turn(i, _):
        x_now = (i == 0) != x_last
        when(x_now, x_rows)
        when(no(x_now), y_rows)
        return 0

    lax.fori_loop(0, 2, in_turn, 0)

    binned[:, 0:32] += rows((0, 1, 14, 15), (0, 1, 14, 15))

    pl.semaphore_wait(know.at[2], 8)

    def by_step(x, moves):
        moved = x
        for t in range(1, 4):
            moved = jnp.where(step_of == t, pltpu.roll(x, moves[t], 1), moved)
        return moved

    for k in range(8):
        spread = by_step(binned[8 * k : 8 * k + 8, :], (0, 32, 64, 96))
        parts[k] = jnp.sum(spread, axis=0, keepdims=True)

    offsets = [(dy, dz) for dy in range(ny) for dz in range(nz) if dy or dz]
    offsets.sort(key=lambda o: -(min(o[0], ny - o[0]) + min(o[1], nz - o[1]) / 2))
    for i, (dy, dz) in enumerate(offsets):
        peer = near_to(dy, dz)
        remote(parts.at[peer.get("gy", gy)], got.at[i], sent_sem.at[4], came_sem.at[6], peer).start()

    pltpu.make_async_copy(got, got, came_sem.at[6]).wait()
    sums = [parts[gy]] + [got[i] for i in range(len(offsets))]
    while len(sums) > 1:
        sums = [a + b for a, b in zip(sums[::2], sums[1::2])]
    value = sums[0]

    summed[0] = value
    when(x_hi, lambda: pl.semaphore_wait(know.at[3], nx - 1 - gx))
    for d in range(1, nx):
        copy = remote(summed.at[0], got_x.at[d - 1], sent_sem.at[5], came_sem.at[7], {"gx": gx + d})
        when(gx + d < nx, copy.start)
    for n in range(1, nx):
        when(gx == n, pltpu.make_async_copy(got_x.at[0:n], got_x.at[0:n], came_sem.at[7]).wait)
    for d in range(1, nx):
        value = value + jnp.where(gx >= d, got_x[d - 1], 0.0)

    value = jnp.broadcast_to(value, (8, 128))
    value = jnp.where((lane >> 5) >= first, value, 0.0)
    value = value * (0.25 * 256 / (nx * 16 * ny * 16 * nz * 128))
    steps = [pltpu.roll(value, lax.rem(256 - 32 * t - 4 * gz, 128), 1) for t in range(4)]
    value = steps[0]
    for t in range(1, 4):
        value = value + jnp.where(sub >= t, steps[t], 0.0)
    energy_out[0] = value[0:4, 0:4]

    def left(i, ref):
        pltpu.make_async_copy(ref, ref, sent_sem.at[i]).wait()

    flush(sent_sem.at[0], lambda y, z: 8 * z + y * (z + 1))
    flush(sent_sem.at[1], lambda y, z: 32 * y)
    when(x_lo, x_down.wait_send)
    when(x_hi, x_up.wait_send)
    left(4, got)
    for n in range(1, nx):
        when(gx == nx - 1 - n, lambda n=n: left(5, got_x.at[0:n]))


def write(psi, energy, psi_out, energy_out, sem):
    for c in range(CT):
        pltpu.make_async_copy(psi.at[:, :, c], psi_out.at[c], sem.at[0]).start()
    small = pltpu.make_async_copy(energy, energy_out, sem.at[1])
    small.start()
    pltpu.make_async_copy(psi_out, psi_out, sem.at[0]).wait()
    small.wait()


def solution(mesh):
    sizes = tuple(mesh.shape[a] for a in ("gx", "gy", "gz"))
    vmem = pl.BlockSpec(memory_space=pltpu.VMEM)
    hbm = pl.BlockSpec(memory_space=pltpu.HBM)

    def body(strain, cell_shell_index, onset_step):
        psi, energy = pl.pallas_call(
            lambda *refs: kernel(sizes, *refs),
            out_shape=(pltpu.VMEM((16, 16, 8, 128), F32), pltpu.VMEM((1, 4, 4), F32)),
            in_specs=[hbm] * 3,
            out_specs=(vmem, vmem),
            scratch_shapes=[
                pltpu.VMEM((20, 20, 8, 128), F32),
                pltpu.VMEM((16, 16, 128), jnp.int32),
                pltpu.VMEM((2, 128), jnp.int32),
                pltpu.VMEM((10, 8, 128), F32),
                pltpu.VMEM((10, 8, 128), F32),
                pltpu.VMEM((10, 8, 128), F32),
                pltpu.VMEM((16, 16, 128), jnp.int32),
                pltpu.VMEM((16, 16, 128), jnp.int32),
                pltpu.VMEM((16, 20, 8, 128), F32),
                pltpu.VMEM((16, 16, 8, 128), F32),
                pltpu.VMEM((64, 128), F32),
                pltpu.VMEM((8, 1, 128), F32),
                pltpu.VMEM((63, 1, 128), F32),
                pltpu.VMEM((7, 1, 128), F32),
                pltpu.VMEM((1, 1, 128), F32),
                pltpu.SemaphoreType.DMA((4,)),
                pltpu.SemaphoreType.DMA((6,)),
                pltpu.SemaphoreType.DMA((8,)),
                pltpu.SemaphoreType.REGULAR((4,)),
            ],
            compiler_params=pltpu.CompilerParams(collective_id=0, has_side_effects=True),
        )(strain.reshape(8, 16, 16, 128), cell_shell_index, onset_step.reshape(2, 128))
        psi_four, energy = pl.pallas_call(
            write,
            out_shape=(
                jax.ShapeDtypeStruct((8, 16, 16, 128), F32),
                jax.ShapeDtypeStruct((1, 4, 4), F32),
            ),
            in_specs=[vmem] * 2,
            out_specs=(hbm, hbm),
            scratch_shapes=[pltpu.SemaphoreType.DMA((2,))],
        )(*(pltpu.with_memory_space_constraint(a, pltpu.VMEM) for a in (psi, energy)))
        return psi_four.reshape(strain.shape), energy

    placed = (P(None, None, "gx", "gy", "gz"), P("gx", "gy", "gz"), P())
    return jax.shard_map(
        body,
        mesh=mesh,
        in_specs=placed,
        out_specs=(P(None, None, "gx", "gy", "gz"), P("gx", None, ("gy", "gz"))),
        check_vma=False,
    )
```

```python
import jax
import jax.numpy as jnp
from jax import lax
from jax.experimental import pallas as pl
from jax.experimental.pallas import tpu as pltpu
from jax.sharding import PartitionSpec as P

MESH = pl.DeviceIdType.MESH
F32 = jnp.float32
CT = 8


def kernel(
    sizes,
    strain,
    shells,
    onset,
    psi_out,
    energy_out,
    field,
    shell,
    onsets,
    zmid,
    zlow,
    zhigh,
    outer,
    inner,
    firsts,
    seconds,
    binned,
    parts,
    got,
    got_x,
    summed,
    in_sem,
    sent_sem,
    came_sem,
    know,
):
    nx, ny, nz = sizes
    gx, gy, gz = (lax.axis_index(a) for a in ("gx", "gy", "gz"))
    no = jnp.logical_not
    both = jnp.logical_and

    def when(cond, act):
        if cond is None:
            act()
        else:
            pl.when(cond)(act)

    def tell(sem, peer, cond=None):
        when(cond, lambda: pl.semaphore_signal(sem, inc=1, device_id=peer, device_id_type=MESH))

    def total_of(conds):
        return sum(c.astype(jnp.int32) for c in conds)

    def near_to(dy, dz):
        peer = {}
        if dy:
            peer["gy"] = lax.rem(gy + (dy + ny), ny)
        if dz:
            peer["gz"] = lax.rem(gz + (dz + nz), nz)
        return peer

    around = [(dy, dz) for dy in (-1, 0, 1) for dz in (-1, 0, 1) if dy or dz]

    barrier = pltpu.get_barrier_semaphore()
    x_lo, x_hi = gx > 0, gx < nx - 1
    y_lo, y_hi = gy > 0, gy < ny - 1
    z_lo, z_hi = gz > 0, gz < nz - 1
    half = nx // 2
    late, soon = both(x_hi, gx < half), both(x_hi, gx >= half)
    tell(barrier, {"gx": gx - 1}, gx > half)
    for step in around:
        tell(barrier, near_to(*step))
    for d in range(1, nx):
        tell(barrier, {"gx": gx + d}, gx + d < nx)
    greeted = 8 + gx + total_of((soon,))

    for h in range(4):
        for c in range(CT):
            pltpu.make_async_copy(
                strain.at[c, 4 * h : 4 * h + 4],
                field.at[4 * h + 2 : 4 * h + 6, 2:18, c],
                in_sem.at[h // 2],
            ).start()
    labels = pltpu.make_async_copy(shells, shell, in_sem.at[2])
    starts = pltpu.make_async_copy(onset, onsets, in_sem.at[3])
    labels.start()
    starts.start()

    def zero(cond, ref):
        @pl.when(cond)
        def _():
            ref[...] = jnp.zeros(ref.shape, F32)

    zero(no(x_lo), field.at[0:2, 2:18])
    zero(no(x_hi), field.at[18:20, 2:18])
    zero(no(y_lo), field.at[2:18, 0:2])
    zero(no(y_hi), field.at[2:18, 18:20])
    zero(no(y_lo), zmid.at[0])
    zero(no(y_hi), zmid.at[9])
    zero(no(z_lo), zlow.at[1:9])
    zero(no(z_hi), zhigh.at[1:9])
    zero(no(both(y_lo, z_lo)), zlow.at[0])
    zero(no(both(y_hi, z_lo)), zlow.at[9])
    zero(no(both(y_lo, z_hi)), zhigh.at[0])
    zero(no(both(y_hi, z_hi)), zhigh.at[9])

    lane = lax.broadcasted_iota(jnp.int32, (8, 128), 1)
    sub = lax.broadcasted_iota(jnp.int32, (8, 128), 0)
    slot_of = ((lane + 2) & 127) >> 2
    quarter = lane & 3

    for h in range(2):
        own = field.at[8 * h + 2 : 8 * h + 10, 2:18]
        pltpu.make_async_copy(own, own, in_sem.at[h]).wait()

    def pack(bs):
        packed = {b: jnp.zeros((8, 128), F32) for b in bs}
        for s in range(32):
            mine = slot_of == s
            for b in bs:
                row = field[s // 2 + 2, 2 * b + s % 2 + 2]
                moved = pltpu.roll(row, 4 * s, 1) if s else row
                packed[b] = jnp.where(mine, moved, packed[b])
        for b in bs:
            zmid[b + 1] = packed[b]

    pack((0, 7))

    pl.semaphore_wait(barrier, greeted)

    tell(know.at[0], {"gx": gx - 1}, both(x_lo, gx <= half))
    for step in around:
        tell(know.at[1], near_to(*step))
    for d in range(1, nx):
        tell(know.at[3], {"gx": gx - d}, gx >= d)

    def remote(src, dst, send, recv, peer):
        return pltpu.make_async_remote_copy(
            src_ref=src, dst_ref=dst, send_sem=send, recv_sem=recv, device_id=peer, device_id_type=MESH
        )

    halos = [
        (zmid.at[1:9], zlow.at[1:9], (0, 1), 0),
        (zmid.at[1:9], zhigh.at[1:9], (0, -1), 0),
        (zmid.at[8], zlow.at[0], (1, 1), 1),
        (zmid.at[8], zhigh.at[0], (1, -1), 1),
        (zmid.at[1], zlow.at[9], (-1, 1), 1),
        (zmid.at[1], zhigh.at[9], (-1, -1), 1),
        (zmid.at[8], zmid.at[0], (1, 0), 1),
        (zmid.at[1], zmid.at[9], (-1, 0), 1),
    ]
    def send(halos):
        for src, dst, (dy, dz), i in halos:
            is_there = {(0, 1): z_hi, (0, -1): z_lo, (1, 0): y_hi, (-1, 0): y_lo}
            there = is_there.get((dy, dz))
            if there is None:
                there = both(is_there[dy, 0], is_there[0, dz])
            when(there, remote(src, dst, sent_sem.at[i // 2], came_sem.at[i], near_to(dy, dz)).start)
    y_halos = []
    for h in range(2):
        mine = pl.ds(8 * h + 2, 8)
        y_halos.append((field.at[mine, 16:18], field.at[mine, 0:2], (1, 0), 2 + h))
        y_halos.append((field.at[mine, 2:4], field.at[mine, 18:20], (-1, 0), 2 + h))
    send(halos[2:])
    send(y_halos)
    y_two, z_two = both(y_lo, y_hi), both(z_lo, z_hi)

    def flush(sem, tiles):
        for y_count in (1, 2):
            for z_count in (1, 2):
                n = tiles(y_count, z_count)
                ref = field.at[0, 0:n] if n <= 20 else field.at[0:4, 0 : n // 4] if n % 4 == 0 else field.at[0:2, 0 : n // 2]
                wait = pltpu.make_async_copy(ref, ref, sem).wait
                when(both(y_two if y_count == 2 else no(y_two), z_two if z_count == 2 else no(z_two)), wait)

    x_down = remote(
        field.at[2:4, 2:18], field.at[18:20, 2:18], sent_sem.at[2], came_sem.at[4], {"gx": gx - 1}
    )
    x_up = remote(
        field.at[16:18, 2:18], field.at[0:2, 2:18], sent_sem.at[3], came_sem.at[5], {"gx": gx + 1}
    )
    when(x_lo, x_down.start)
    when(soon, x_up.start)
    pack(range(1, 7))
    send(halos[:2])

    labels.wait()
    starts.wait()
    outer[...] = shell[...] >> 5
    inner[...] = shell[...] & 31
    first = jnp.broadcast_to(onsets[pl.ds(gy // 4, 1), :], (8, 128))
    first = pltpu.roll(first, lax.rem(128 - 32 * lax.rem(gy, 4), 128), 1)
    first = jnp.where(lane < 32, first, 0)
    first = first + pltpu.roll(first, 32, 1)
    first = first + pltpu.roll(first, 64, 1)

    signs = jnp.where(sub < 4, 1.0 / 24.0, -1.0 / 24.0).astype(F32)
    minus = -signs

    def shifts(f):
        return (pltpu.roll(f, k, 1) for k in (127, 126, 1, 2))

    def slope(up1, up2, down1, down2):
        d = (up1 - down1) * (8.0 / 144.0) - (up2 - down2) * (1.0 / 144.0)
        return pltpu.roll(d, 4, 0)

    def stars(x, y):
        near = (field[x + 1, y + 2] + field[x + 3, y + 2]) + (field[x + 2, y + 1] + field[x + 2, y + 3])
        far = (field[x, y + 2] + field[x + 4, y + 2]) + (field[x + 2, y] + field[x + 2, y + 4])
        return (16.0 * near - far) * signs

    def along_z(xs, whole):
        for x in xs:
            for y in range(16):
                f = field[x + 2, y + 2]
                up1, up2, down1, down2 = shifts(f)
                firsts[x, y + 2] = slope(up1, up2, down1, down2)
                bend = 16.0 * (up1 + down1) - (up2 + down2)
                value = (bend + 30.0 * f) * minus
                if whole and 2 <= y < 14:
                    value = value + stars(x, y)
                seconds[x, y] = value
        return 0

    lax.fori_loop(0, 3, lambda i, _: along_z([4 * i + 2 + j for j in range(4)], True), 0)
    lax.fori_loop(0, 2, lambda i, _: along_z([14 * i, 14 * i + 1], False), 0)

    flush(came_sem.at[0], lambda y, z: 8 * z)

    pl.semaphore_wait(know.at[1], 8)
    for dy, dz in around:
        tell(know.at[2], near_to(2 * dy, 2 * dz))

    when(late, lambda: pl.semaphore_wait(know.at[0], 1))
    when(late, x_up.start)

    even = (slot_of & 1) == 0
    at_end = jnp.logical_or(lane < 2, lane >= 126)
    turns = {}

    def turn(b):
        wrong = jnp.where(quarter >= 2, zlow[b], zhigh[b]) - zmid[b]
        near = jnp.where(
            quarter == 0, pltpu.roll(wrong, 1, 1), jnp.where(quarter == 3, pltpu.roll(wrong, 127, 1), 0.0)
        )
        far = jnp.where(quarter < 2, pltpu.roll(wrong, 2, 1), pltpu.roll(wrong, 126, 1))
        error = far - 8.0 * near
        error = jnp.where(quarter < 2, error, -error)
        turns[b] = (error, pltpu.roll(error, 124, 1), pltpu.roll(error, 4, 1), 16.0 * near - far)

    def mend(b):
        (before, before_up, _, _), (_, up, down, bend), (after, _, after_down, _) = (
            turns[b - 1],
            turns[b],
            turns[b + 1],
        )
        step1 = jnp.where(even, up - before_up, after_down - down)
        mixed = 8.0 * step1 - (after - before)
        fix = bend * minus - pltpu.roll(mixed, 4, 0) * (1.0 / 144.0)
        for s in range(32):
            x, y = s // 2, 2 * b - 2 + s % 2
            end = pltpu.roll(fix, 128 - 4 * s, 1) if s else fix
            seconds[x, y] = seconds[x, y] + jnp.where(at_end, end, 0.0)

    for b in range(1, 9):
        turn(b)
    for b in range(2, 8):
        mend(b)

    step_of = sub & 3
    uz = (lane + gz * 128).astype(F32)
    uz = (uz + 0.5) / (nz * 128) - 0.5
    uz2 = (uz * uz + 0.05) * 0.0625

    def rows(xs, ys, whole=False):
        lefts, rights = [], []
        for x in xs:
            ux = (x + gx * 16).astype(F32)
            ux = (ux + 0.5) / (nx * 16) - 0.5
            ux2 = uz2 + ux * ux * 0.0625
            for y in ys:
                mixed = 8.0 * (firsts[x, y + 3] - firsts[x, y + 1]) - (firsts[x, y + 4] - firsts[x, y])
                value = seconds[x, y] - mixed
                if not whole:
                    value = value + stars(x, y)
                psi_out[x, y] = value
                news = value + jnp.where(step_of >= 1, pltpu.roll(value, 1, 0), 0.0)
                news = news + jnp.where(step_of >= 2, pltpu.roll(news, 2, 0), 0.0)
                power = news * news
                power = power + pltpu.roll(power, 4, 0)
                uy = (gy * 16 + y).astype(F32)
                uy = (uy + 0.5) / (ny * 16) - 0.5
                flux = power * (ux2 + uy * uy * 0.0625)
                high = flux.astype(jnp.bfloat16).astype(F32)
                split = jnp.where(sub < 4, high, flux - high)
                high_label = jnp.broadcast_to(outer[x, pl.ds(y, 1), :], (8, 128))
                low_label = jnp.broadcast_to(inner[x, pl.ds(y, 1), :], (8, 128))
                lefts.append(
                    jnp.concatenate([jnp.where(high_label == k, split, 0.0) for k in range(8)], axis=0)
                )
                rights.append(
                    jnp.concatenate(
                        [jnp.where(low_label == sub + 8 * j, 1.0, 0.0).astype(F32) for j in range(4)], axis=0
                    )
                )
        left = jnp.concatenate(lefts, axis=1)
        right = jnp.concatenate(rights, axis=1)
        return lax.dot_general(left, right, (((1,), (1,)), ((), ())), preferred_element_type=F32)

    total = lax.fori_loop(
        0,
        4,
        lambda i, t: t + rows([3 * i + 2 + j for j in range(3)], range(2, 14), True),
        jnp.zeros((64, 32), F32),
    )
    binned[...] = jnp.zeros((64, 128), F32)
    binned[:, 0:32] = total

    def x_rows():
        when(x_hi, x_down.wait_recv)
        when(x_lo, x_up.wait_recv)
        binned[:, 0:32] += rows((0, 1, 14, 15), range(2, 14))

    x_last = jnp.logical_or(gx == half - 1, gx == half)

    def y_rows():
        flush(came_sem.at[1], lambda y, z: y * (z + 1))
        flush(came_sem.at[2], lambda y, z: 16 * y)

        def y_ends(xs):
            for x in xs:
                for y in (0, 1, 18, 19):
                    up1, up2, down1, down2 = shifts(field[x + 2, y])
                    firsts[x, y] = slope(up1, up2, down1, down2)

        y_ends(range(8))
        for b in (0, 1, 2, 7, 8, 9):
            turn(b)
        for b in (1, 8):
            mend(b)
        binned[:, 0:32] += rows(range(2, 8), (0, 1, 14, 15))
        flush(came_sem.at[3], lambda y, z: 16 * y)
        y_ends(range(8, 16))
        binned[:, 0:32] += rows(range(8, 14), (0, 1, 14, 15))

    def in_turn(i, _):
        x_now = (i == 0) != x_last
        when(x_now, x_rows)
        when(no(x_now), y_rows)
        return 0

    lax.fori_loop(0, 2, in_turn, 0)

    binned[:, 0:32] += rows((0, 1, 14, 15), (0, 1, 14, 15))

    pl.semaphore_wait(know.at[2], 8)

    def by_step(x, moves):
        moved = x
        for t in range(1, 4):
            moved = jnp.where(step_of == t, pltpu.roll(x, moves[t], 1), moved)
        return moved

    for k in range(8):
        spread = by_step(binned[8 * k : 8 * k + 8, :], (0, 32, 64, 96))
        parts[k] = jnp.sum(spread, axis=0, keepdims=True)

    offsets = [(dy, dz) for dy in range(ny) for dz in range(nz) if dy or dz]
    offsets.sort(key=lambda o: -(min(o[0], ny - o[0]) + min(o[1], nz - o[1]) / 2))
    for i, (dy, dz) in enumerate(offsets):
        peer = near_to(dy, dz)
        remote(parts.at[peer.get("gy", gy)], got.at[i], sent_sem.at[4], came_sem.at[6], peer).start()

    pltpu.make_async_copy(got, got, came_sem.at[6]).wait()
    sums = [parts[gy]] + [got[i] for i in range(len(offsets))]
    while len(sums) > 1:
        sums = [a + b for a, b in zip(sums[::2], sums[1::2])]
    value = sums[0]

    summed[0] = value
    when(x_hi, lambda: pl.semaphore_wait(know.at[3], nx - 1 - gx))
    for d in range(1, nx):
        copy = remote(summed.at[0], got_x.at[d - 1], sent_sem.at[5], came_sem.at[7], {"gx": gx + d})
        when(gx + d < nx, copy.start)
    for n in range(1, nx):
        when(gx == n, pltpu.make_async_copy(got_x.at[0:n], got_x.at[0:n], came_sem.at[7]).wait)
    for d in range(1, nx):
        value = value + jnp.where(gx >= d, got_x[d - 1], 0.0)

    value = jnp.broadcast_to(value, (8, 128))
    value = jnp.where((lane >> 5) >= first, value, 0.0)
    value = value * (0.25 * 256 / (nx * 16 * ny * 16 * nz * 128))
    steps = [pltpu.roll(value, lax.rem(256 - 32 * t - 4 * gz, 128), 1) for t in range(4)]
    value = steps[0]
    for t in range(1, 4):
        value = value + jnp.where(sub >= t, steps[t], 0.0)
    energy_out[0] = value[0:4, 0:4]

    def left(i, ref):
        pltpu.make_async_copy(ref, ref, sent_sem.at[i]).wait()

    flush(sent_sem.at[0], lambda y, z: 8 * z + y * (z + 1))
    flush(sent_sem.at[1], lambda y, z: 32 * y)
    when(x_lo, x_down.wait_send)
    when(x_hi, x_up.wait_send)
    left(4, got)
    for n in range(1, nx):
        when(gx == nx - 1 - n, lambda n=n: left(5, got_x.at[0:n]))


def write(psi, energy, psi_out, energy_out, sem):
    for c in range(CT):
        for h in range(4):
            mine = pl.ds(4 * h, 4)
            pltpu.make_async_copy(psi.at[mine, :, c], psi_out.at[c, mine], sem.at[0]).start()
    small = pltpu.make_async_copy(energy, energy_out, sem.at[1])
    small.start()
    pltpu.make_async_copy(psi_out, psi_out, sem.at[0]).wait()
    small.wait()


def solution(mesh):
    sizes = tuple(mesh.shape[a] for a in ("gx", "gy", "gz"))
    vmem = pl.BlockSpec(memory_space=pltpu.VMEM)
    hbm = pl.BlockSpec(memory_space=pltpu.HBM)

    def body(strain, cell_shell_index, onset_step):
        psi, energy = pl.pallas_call(
            lambda *refs: kernel(sizes, *refs),
            out_shape=(pltpu.VMEM((16, 16, 8, 128), F32), pltpu.VMEM((1, 4, 4), F32)),
            in_specs=[hbm] * 3,
            out_specs=(vmem, vmem),
            scratch_shapes=[
                pltpu.VMEM((20, 20, 8, 128), F32),
                pltpu.VMEM((16, 16, 128), jnp.int32),
                pltpu.VMEM((2, 128), jnp.int32),
                pltpu.VMEM((10, 8, 128), F32),
                pltpu.VMEM((10, 8, 128), F32),
                pltpu.VMEM((10, 8, 128), F32),
                pltpu.VMEM((16, 16, 128), jnp.int32),
                pltpu.VMEM((16, 16, 128), jnp.int32),
                pltpu.VMEM((16, 20, 8, 128), F32),
                pltpu.VMEM((16, 16, 8, 128), F32),
                pltpu.VMEM((64, 128), F32),
                pltpu.VMEM((8, 1, 128), F32),
                pltpu.VMEM((63, 1, 128), F32),
                pltpu.VMEM((7, 1, 128), F32),
                pltpu.VMEM((1, 1, 128), F32),
                pltpu.SemaphoreType.DMA((4,)),
                pltpu.SemaphoreType.DMA((6,)),
                pltpu.SemaphoreType.DMA((8,)),
                pltpu.SemaphoreType.REGULAR((4,)),
            ],
            compiler_params=pltpu.CompilerParams(collective_id=0, has_side_effects=True),
        )(strain.reshape(8, 16, 16, 128), cell_shell_index, onset_step.reshape(2, 128))
        psi_four, energy = pl.pallas_call(
            write,
            out_shape=(
                jax.ShapeDtypeStruct((8, 16, 16, 128), F32),
                jax.ShapeDtypeStruct((1, 4, 4), F32),
            ),
            in_specs=[vmem] * 2,
            out_specs=(hbm, hbm),
            scratch_shapes=[pltpu.SemaphoreType.DMA((2,))],
        )(*(pltpu.with_memory_space_constraint(a, pltpu.VMEM) for a in (psi, energy)))
        return psi_four.reshape(strain.shape), energy

    placed = (P(None, None, "gx", "gy", "gz"), P("gx", "gy", "gz"), P())
    return jax.shard_map(
        body,
        mesh=mesh,
        in_specs=placed,
        out_specs=(P(None, None, "gx", "gy", "gz"), P("gx", None, ("gy", "gz"))),
        check_vma=False,
    )
```

```python
import jax
import jax.numpy as jnp
from jax import lax
from jax.experimental import pallas as pl
from jax.experimental.pallas import tpu as pltpu
from jax.sharding import PartitionSpec as P

MESH = pl.DeviceIdType.MESH
F32 = jnp.float32
CT = 8


def kernel(
    sizes,
    strain,
    shells,
    onset,
    psi_out,
    energy_out,
    field,
    shell,
    onsets,
    zmid,
    zlow,
    zhigh,
    outer,
    inner,
    firsts,
    seconds,
    binned,
    parts,
    got,
    got_x,
    summed,
    in_sem,
    sent_sem,
    came_sem,
    know,
):
    nx, ny, nz = sizes
    gx, gy, gz = (lax.axis_index(a) for a in ("gx", "gy", "gz"))
    no = jnp.logical_not
    both = jnp.logical_and

    def when(cond, act):
        if cond is None:
            act()
        else:
            pl.when(cond)(act)

    def tell(sem, peer, cond=None):
        when(cond, lambda: pl.semaphore_signal(sem, inc=1, device_id=peer, device_id_type=MESH))

    def total_of(conds):
        return sum(c.astype(jnp.int32) for c in conds)

    def near_to(dy, dz):
        peer = {}
        if dy:
            peer["gy"] = lax.rem(gy + (dy + ny), ny)
        if dz:
            peer["gz"] = lax.rem(gz + (dz + nz), nz)
        return peer

    around = [(dy, dz) for dy in (-1, 0, 1) for dz in (-1, 0, 1) if dy or dz]

    barrier = pltpu.get_barrier_semaphore()
    x_lo, x_hi = gx > 0, gx < nx - 1
    y_lo, y_hi = gy > 0, gy < ny - 1
    z_lo, z_hi = gz > 0, gz < nz - 1
    half = nx // 2
    late, soon = both(x_hi, gx < half), both(x_hi, gx >= half)
    tell(barrier, {"gx": gx - 1}, gx > half)
    for step in around:
        tell(barrier, near_to(*step))
    for d in range(1, nx):
        tell(barrier, {"gx": gx + d}, gx + d < nx)
    greeted = 8 + gx + total_of((soon,))

    for h in range(4):
        for c in range(CT):
            pltpu.make_async_copy(
                strain.at[c, 4 * h : 4 * h + 4],
                field.at[4 * h + 2 : 4 * h + 6, 2:18, c],
                in_sem.at[h // 2],
            ).start()
    labels = pltpu.make_async_copy(shells, shell, in_sem.at[2])
    starts = pltpu.make_async_copy(onset, onsets, in_sem.at[3])
    labels.start()
    starts.start()

    def zero(cond, ref):
        @pl.when(cond)
        def _():
            ref[...] = jnp.zeros(ref.shape, F32)

    zero(no(x_lo), field.at[0:2, 2:18])
    zero(no(x_hi), field.at[18:20, 2:18])
    zero(no(y_lo), field.at[2:18, 0:2])
    zero(no(y_hi), field.at[2:18, 18:20])
    zero(no(y_lo), zmid.at[0])
    zero(no(y_hi), zmid.at[9])
    zero(no(z_lo), zlow.at[1:9])
    zero(no(z_hi), zhigh.at[1:9])
    zero(no(both(y_lo, z_lo)), zlow.at[0])
    zero(no(both(y_hi, z_lo)), zlow.at[9])
    zero(no(both(y_lo, z_hi)), zhigh.at[0])
    zero(no(both(y_hi, z_hi)), zhigh.at[9])

    lane = lax.broadcasted_iota(jnp.int32, (8, 128), 1)
    sub = lax.broadcasted_iota(jnp.int32, (8, 128), 0)
    slot_of = ((lane + 2) & 127) >> 2
    quarter = lane & 3

    for h in range(2):
        own = field.at[8 * h + 2 : 8 * h + 10, 2:18]
        pltpu.make_async_copy(own, own, in_sem.at[h]).wait()

    def pack(bs):
        packed = {b: jnp.zeros((8, 128), F32) for b in bs}
        for s in range(32):
            mine = slot_of == s
            for b in bs:
                row = field[s // 2 + 2, 2 * b + s % 2 + 2]
                moved = pltpu.roll(row, 4 * s, 1) if s else row
                packed[b] = jnp.where(mine, moved, packed[b])
        for b in bs:
            zmid[b + 1] = packed[b]

    pack((0, 7))

    pl.semaphore_wait(barrier, greeted)

    tell(know.at[0], {"gx": gx - 1}, both(x_lo, gx <= half))
    for step in around:
        tell(know.at[1], near_to(*step))
    for d in range(1, nx):
        tell(know.at[3], {"gx": gx - d}, gx >= d)

    def remote(src, dst, send, recv, peer):
        return pltpu.make_async_remote_copy(
            src_ref=src, dst_ref=dst, send_sem=send, recv_sem=recv, device_id=peer, device_id_type=MESH
        )

    halos = [
        (zmid.at[1:9], zlow.at[1:9], (0, 1), 0),
        (zmid.at[1:9], zhigh.at[1:9], (0, -1), 0),
        (zmid.at[8], zlow.at[0], (1, 1), 1),
        (zmid.at[8], zhigh.at[0], (1, -1), 1),
        (zmid.at[1], zlow.at[9], (-1, 1), 1),
        (zmid.at[1], zhigh.at[9], (-1, -1), 1),
        (zmid.at[8], zmid.at[0], (1, 0), 1),
        (zmid.at[1], zmid.at[9], (-1, 0), 1),
    ]
    def send(halos):
        for src, dst, (dy, dz), i in halos:
            is_there = {(0, 1): z_hi, (0, -1): z_lo, (1, 0): y_hi, (-1, 0): y_lo}
            there = is_there.get((dy, dz))
            if there is None:
                there = both(is_there[dy, 0], is_there[0, dz])
            when(there, remote(src, dst, sent_sem.at[i // 2], came_sem.at[i], near_to(dy, dz)).start)
    y_halos = []
    for h in range(2):
        mine = pl.ds(8 * h + 2, 8)
        y_halos.append((field.at[mine, 16:18], field.at[mine, 0:2], (1, 0), 2 + h))
        y_halos.append((field.at[mine, 2:4], field.at[mine, 18:20], (-1, 0), 2 + h))
    send(halos[2:])
    send(y_halos)
    y_two, z_two = both(y_lo, y_hi), both(z_lo, z_hi)

    def flush(sem, tiles):
        for y_count in (1, 2):
            for z_count in (1, 2):
                n = tiles(y_count, z_count)
                ref = field.at[0, 0:n] if n <= 20 else field.at[0:4, 0 : n // 4] if n % 4 == 0 else field.at[0:2, 0 : n // 2]
                wait = pltpu.make_async_copy(ref, ref, sem).wait
                when(both(y_two if y_count == 2 else no(y_two), z_two if z_count == 2 else no(z_two)), wait)

    x_down = remote(
        field.at[2:4, 2:18], field.at[18:20, 2:18], sent_sem.at[2], came_sem.at[4], {"gx": gx - 1}
    )
    x_up = remote(
        field.at[16:18, 2:18], field.at[0:2, 2:18], sent_sem.at[3], came_sem.at[5], {"gx": gx + 1}
    )
    when(x_lo, x_down.start)
    when(soon, x_up.start)
    pack(range(1, 7))
    send(halos[:2])

    labels.wait()
    starts.wait()
    outer[...] = shell[...] >> 5
    inner[...] = shell[...] & 31
    first = jnp.broadcast_to(onsets[pl.ds(gy // 4, 1), :], (8, 128))
    first = pltpu.roll(first, lax.rem(128 - 32 * lax.rem(gy, 4), 128), 1)
    first = jnp.where(lane < 32, first, 0)
    first = first + pltpu.roll(first, 32, 1)
    first = first + pltpu.roll(first, 64, 1)

    signs = jnp.where(sub < 4, 1.0 / 24.0, -1.0 / 24.0).astype(F32)
    minus = -signs

    def shifts(f):
        return (pltpu.roll(f, k, 1) for k in (127, 126, 1, 2))

    def slope(up1, up2, down1, down2):
        d = (up1 - down1) * (8.0 / 144.0) - (up2 - down2) * (1.0 / 144.0)
        return pltpu.roll(d, 4, 0)

    def stars(x, y):
        near = (field[x + 1, y + 2] + field[x + 3, y + 2]) + (field[x + 2, y + 1] + field[x + 2, y + 3])
        far = (field[x, y + 2] + field[x + 4, y + 2]) + (field[x + 2, y] + field[x + 2, y + 4])
        return (16.0 * near - far) * signs

    def along_z(xs, whole):
        for x in xs:
            for y in range(16):
                f = field[x + 2, y + 2]
                up1, up2, down1, down2 = shifts(f)
                firsts[x, y + 2] = slope(up1, up2, down1, down2)
                bend = 16.0 * (up1 + down1) - (up2 + down2)
                value = (bend + 30.0 * f) * minus
                if whole and 2 <= y < 14:
                    value = value + stars(x, y)
                seconds[x, y] = value
        return 0

    lax.fori_loop(0, 3, lambda i, _: along_z([4 * i + 2 + j for j in range(4)], True), 0)
    lax.fori_loop(0, 2, lambda i, _: along_z([14 * i, 14 * i + 1], False), 0)

    when(late, lambda: pl.semaphore_wait(know.at[0], 1))
    when(late, x_up.start)

    flush(came_sem.at[0], lambda y, z: 8 * z)

    pl.semaphore_wait(know.at[1], 8)
    for dy, dz in around:
        tell(know.at[2], near_to(2 * dy, 2 * dz))

    even = (slot_of & 1) == 0
    at_end = jnp.logical_or(lane < 2, lane >= 126)
    turns = {}

    def turn(b):
        wrong = jnp.where(quarter >= 2, zlow[b], zhigh[b]) - zmid[b]
        near = jnp.where(
            quarter == 0, pltpu.roll(wrong, 1, 1), jnp.where(quarter == 3, pltpu.roll(wrong, 127, 1), 0.0)
        )
        far = jnp.where(quarter < 2, pltpu.roll(wrong, 2, 1), pltpu.roll(wrong, 126, 1))
        error = far - 8.0 * near
        error = jnp.where(quarter < 2, error, -error)
        turns[b] = (error, pltpu.roll(error, 124, 1), pltpu.roll(error, 4, 1), 16.0 * near - far)

    def mend(b):
        (before, before_up, _, _), (_, up, down, bend), (after, _, after_down, _) = (
            turns[b - 1],
            turns[b],
            turns[b + 1],
        )
        step1 = jnp.where(even, up - before_up, after_down - down)
        mixed = 8.0 * step1 - (after - before)
        fix = bend * minus - pltpu.roll(mixed, 4, 0) * (1.0 / 144.0)
        for s in range(32):
            x, y = s // 2, 2 * b - 2 + s % 2
            end = pltpu.roll(fix, 128 - 4 * s, 1) if s else fix
            seconds[x, y] = seconds[x, y] + jnp.where(at_end, end, 0.0)

    for b in range(1, 9):
        turn(b)
    for b in range(2, 8):
        mend(b)

    step_of = sub & 3
    uz = (lane + gz * 128).astype(F32)
    uz = (uz + 0.5) / (nz * 128) - 0.5
    uz2 = (uz * uz + 0.05) * 0.0625

    def rows(xs, ys, whole=False):
        lefts, rights = [], []
        for x in xs:
            ux = (x + gx * 16).astype(F32)
            ux = (ux + 0.5) / (nx * 16) - 0.5
            ux2 = uz2 + ux * ux * 0.0625
            for y in ys:
                mixed = 8.0 * (firsts[x, y + 3] - firsts[x, y + 1]) - (firsts[x, y + 4] - firsts[x, y])
                value = seconds[x, y] - mixed
                if not whole:
                    value = value + stars(x, y)
                psi_out[x, y] = value
                news = value + jnp.where(step_of >= 1, pltpu.roll(value, 1, 0), 0.0)
                news = news + jnp.where(step_of >= 2, pltpu.roll(news, 2, 0), 0.0)
                power = news * news
                power = power + pltpu.roll(power, 4, 0)
                uy = (gy * 16 + y).astype(F32)
                uy = (uy + 0.5) / (ny * 16) - 0.5
                flux = power * (ux2 + uy * uy * 0.0625)
                high = flux.astype(jnp.bfloat16).astype(F32)
                split = jnp.where(sub < 4, high, flux - high)
                high_label = jnp.broadcast_to(outer[x, pl.ds(y, 1), :], (8, 128))
                low_label = jnp.broadcast_to(inner[x, pl.ds(y, 1), :], (8, 128))
                lefts.append(
                    jnp.concatenate([jnp.where(high_label == k, split, 0.0) for k in range(8)], axis=0)
                )
                rights.append(
                    jnp.concatenate(
                        [jnp.where(low_label == sub + 8 * j, 1.0, 0.0).astype(F32) for j in range(4)], axis=0
                    )
                )
        left = jnp.concatenate(lefts, axis=1)
        right = jnp.concatenate(rights, axis=1)
        return lax.dot_general(left, right, (((1,), (1,)), ((), ())), preferred_element_type=F32)

    total = lax.fori_loop(
        0,
        4,
        lambda i, t: t + rows([3 * i + 2 + j for j in range(3)], range(2, 14), True),
        jnp.zeros((64, 32), F32),
    )
    binned[...] = jnp.zeros((64, 128), F32)
    binned[:, 0:32] = total

    def x_rows():
        when(x_hi, x_down.wait_recv)
        when(x_lo, x_up.wait_recv)
        binned[:, 0:32] += rows((0, 1, 14, 15), range(2, 14))

    x_last = jnp.logical_or(gx == half - 1, gx == half)

    def y_rows():
        flush(came_sem.at[1], lambda y, z: y * (z + 1))
        flush(came_sem.at[2], lambda y, z: 16 * y)

        def y_ends(xs):
            for x in xs:
                for y in (0, 1, 18, 19):
                    up1, up2, down1, down2 = shifts(field[x + 2, y])
                    firsts[x, y] = slope(up1, up2, down1, down2)

        y_ends(range(8))
        for b in (0, 1, 2, 7, 8, 9):
            turn(b)
        for b in (1, 8):
            mend(b)
        binned[:, 0:32] += rows(range(2, 8), (0, 1, 14, 15))
        flush(came_sem.at[3], lambda y, z: 16 * y)
        y_ends(range(8, 16))
        binned[:, 0:32] += rows(range(8, 14), (0, 1, 14, 15))

    def in_turn(i, _):
        x_now = (i == 0) != x_last
        when(x_now, x_rows)
        when(no(x_now), y_rows)
        return 0

    lax.fori_loop(0, 2, in_turn, 0)

    binned[:, 0:32] += rows((0, 1, 14, 15), (0, 1, 14, 15))

    pl.semaphore_wait(know.at[2], 8)

    def by_step(x, moves):
        moved = x
        for t in range(1, 4):
            moved = jnp.where(step_of == t, pltpu.roll(x, moves[t], 1), moved)
        return moved

    for k in range(8):
        spread = by_step(binned[8 * k : 8 * k + 8, :], (0, 32, 64, 96))
        parts[k] = jnp.sum(spread, axis=0, keepdims=True)

    offsets = [(dy, dz) for dy in range(ny) for dz in range(nz) if dy or dz]
    offsets.sort(key=lambda o: -(min(o[0], ny - o[0]) + min(o[1], nz - o[1]) / 2))
    for i, (dy, dz) in enumerate(offsets):
        peer = near_to(dy, dz)
        remote(parts.at[peer.get("gy", gy)], got.at[i], sent_sem.at[4], came_sem.at[6], peer).start()

    pltpu.make_async_copy(got, got, came_sem.at[6]).wait()
    sums = [parts[gy]] + [got[i] for i in range(len(offsets))]
    while len(sums) > 1:
        sums = [a + b for a, b in zip(sums[::2], sums[1::2])]
    value = sums[0]

    summed[0] = value
    when(x_hi, lambda: pl.semaphore_wait(know.at[3], nx - 1 - gx))
    for d in range(1, nx):
        copy = remote(summed.at[0], got_x.at[d - 1], sent_sem.at[5], came_sem.at[7], {"gx": gx + d})
        when(gx + d < nx, copy.start)
    for n in range(1, nx):
        when(gx == n, pltpu.make_async_copy(got_x.at[0:n], got_x.at[0:n], came_sem.at[7]).wait)
    for d in range(1, nx):
        value = value + jnp.where(gx >= d, got_x[d - 1], 0.0)

    value = jnp.broadcast_to(value, (8, 128))
    value = jnp.where((lane >> 5) >= first, value, 0.0)
    value = value * (0.25 * 256 / (nx * 16 * ny * 16 * nz * 128))
    steps = [pltpu.roll(value, lax.rem(256 - 32 * t - 4 * gz, 128), 1) for t in range(4)]
    value = steps[0]
    for t in range(1, 4):
        value = value + jnp.where(sub >= t, steps[t], 0.0)
    energy_out[0] = value[0:4, 0:4]

    def left(i, ref):
        pltpu.make_async_copy(ref, ref, sent_sem.at[i]).wait()

    flush(sent_sem.at[0], lambda y, z: 8 * z + y * (z + 1))
    flush(sent_sem.at[1], lambda y, z: 32 * y)
    when(x_lo, x_down.wait_send)
    when(x_hi, x_up.wait_send)
    left(4, got)
    for n in range(1, nx):
        when(gx == nx - 1 - n, lambda n=n: left(5, got_x.at[0:n]))


def write(psi, energy, psi_out, energy_out, sem):
    for c in range(CT):
        for h in range(4):
            mine = pl.ds(4 * h, 4)
            pltpu.make_async_copy(psi.at[mine, :, c], psi_out.at[c, mine], sem.at[0]).start()
    small = pltpu.make_async_copy(energy, energy_out, sem.at[1])
    small.start()
    pltpu.make_async_copy(psi_out, psi_out, sem.at[0]).wait()
    small.wait()


def solution(mesh):
    sizes = tuple(mesh.shape[a] for a in ("gx", "gy", "gz"))
    vmem = pl.BlockSpec(memory_space=pltpu.VMEM)
    hbm = pl.BlockSpec(memory_space=pltpu.HBM)

    def body(strain, cell_shell_index, onset_step):
        psi, energy = pl.pallas_call(
            lambda *refs: kernel(sizes, *refs),
            out_shape=(pltpu.VMEM((16, 16, 8, 128), F32), pltpu.VMEM((1, 4, 4), F32)),
            in_specs=[hbm] * 3,
            out_specs=(vmem, vmem),
            scratch_shapes=[
                pltpu.VMEM((20, 20, 8, 128), F32),
                pltpu.VMEM((16, 16, 128), jnp.int32),
                pltpu.VMEM((2, 128), jnp.int32),
                pltpu.VMEM((10, 8, 128), F32),
                pltpu.VMEM((10, 8, 128), F32),
                pltpu.VMEM((10, 8, 128), F32),
                pltpu.VMEM((16, 16, 128), jnp.int32),
                pltpu.VMEM((16, 16, 128), jnp.int32),
                pltpu.VMEM((16, 20, 8, 128), F32),
                pltpu.VMEM((16, 16, 8, 128), F32),
                pltpu.VMEM((64, 128), F32),
                pltpu.VMEM((8, 1, 128), F32),
                pltpu.VMEM((63, 1, 128), F32),
                pltpu.VMEM((7, 1, 128), F32),
                pltpu.VMEM((1, 1, 128), F32),
                pltpu.SemaphoreType.DMA((4,)),
                pltpu.SemaphoreType.DMA((6,)),
                pltpu.SemaphoreType.DMA((8,)),
                pltpu.SemaphoreType.REGULAR((4,)),
            ],
            compiler_params=pltpu.CompilerParams(collective_id=0, has_side_effects=True),
        )(strain.reshape(8, 16, 16, 128), cell_shell_index, onset_step.reshape(2, 128))
        psi_four, energy = pl.pallas_call(
            write,
            out_shape=(
                jax.ShapeDtypeStruct((8, 16, 16, 128), F32),
                jax.ShapeDtypeStruct((1, 4, 4), F32),
            ),
            in_specs=[vmem] * 2,
            out_specs=(hbm, hbm),
            scratch_shapes=[pltpu.SemaphoreType.DMA((2,))],
        )(*(pltpu.with_memory_space_constraint(a, pltpu.VMEM) for a in (psi, energy)))
        return psi_four.reshape(strain.shape), energy

    placed = (P(None, None, "gx", "gy", "gz"), P("gx", "gy", "gz"), P())
    return jax.shard_map(
        body,
        mesh=mesh,
        in_specs=placed,
        out_specs=(P(None, None, "gx", "gy", "gz"), P("gx", None, ("gy", "gz"))),
        check_vma=False,
    )
```

```python
import jax
import jax.numpy as jnp
from jax import lax
from jax.experimental import pallas as pl
from jax.experimental.pallas import tpu as pltpu
from jax.sharding import PartitionSpec as P

MESH = pl.DeviceIdType.MESH
F32 = jnp.float32
CT = 8


def kernel(
    sizes,
    strain,
    shells,
    onset,
    psi_out,
    energy_out,
    field,
    shell,
    onsets,
    zmid,
    zlow,
    zhigh,
    outer,
    inner,
    firsts,
    seconds,
    binned,
    parts,
    got,
    got_x,
    summed,
    in_sem,
    sent_sem,
    came_sem,
    know,
):
    nx, ny, nz = sizes
    gx, gy, gz = (lax.axis_index(a) for a in ("gx", "gy", "gz"))
    no = jnp.logical_not
    both = jnp.logical_and

    def when(cond, act):
        if cond is None:
            act()
        else:
            pl.when(cond)(act)

    def tell(sem, peer, cond=None):
        when(cond, lambda: pl.semaphore_signal(sem, inc=1, device_id=peer, device_id_type=MESH))

    def total_of(conds):
        return sum(c.astype(jnp.int32) for c in conds)

    def near_to(dy, dz):
        peer = {}
        if dy:
            peer["gy"] = lax.rem(gy + (dy + ny), ny)
        if dz:
            peer["gz"] = lax.rem(gz + (dz + nz), nz)
        return peer

    around = [(dy, dz) for dy in (-1, 0, 1) for dz in (-1, 0, 1) if dy or dz]

    barrier = pltpu.get_barrier_semaphore()
    x_lo, x_hi = gx > 0, gx < nx - 1
    y_lo, y_hi = gy > 0, gy < ny - 1
    z_lo, z_hi = gz > 0, gz < nz - 1
    half = nx // 2
    late, soon = both(x_hi, gx < half), both(x_hi, gx >= half)
    tell(barrier, {"gx": gx - 1}, gx > half)
    for step in around:
        tell(barrier, near_to(*step))
    for d in range(1, nx):
        tell(barrier, {"gx": gx + d}, gx + d < nx)
    greeted = 8 + gx + total_of((soon,))

    for h in range(4):
        for c in range(CT):
            pltpu.make_async_copy(
                strain.at[c, 4 * h : 4 * h + 4],
                field.at[4 * h + 2 : 4 * h + 6, 2:18, c],
                in_sem.at[h // 2],
            ).start()
    labels = pltpu.make_async_copy(shells, shell, in_sem.at[2])
    starts = pltpu.make_async_copy(onset, onsets, in_sem.at[3])
    labels.start()
    starts.start()

    def zero(cond, ref):
        @pl.when(cond)
        def _():
            ref[...] = jnp.zeros(ref.shape, F32)

    zero(no(x_lo), field.at[0:2, 2:18])
    zero(no(x_hi), field.at[18:20, 2:18])
    zero(no(y_lo), field.at[2:18, 0:2])
    zero(no(y_hi), field.at[2:18, 18:20])
    zero(no(y_lo), zmid.at[0])
    zero(no(y_hi), zmid.at[9])
    zero(no(z_lo), zlow.at[1:9])
    zero(no(z_hi), zhigh.at[1:9])
    zero(no(both(y_lo, z_lo)), zlow.at[0])
    zero(no(both(y_hi, z_lo)), zlow.at[9])
    zero(no(both(y_lo, z_hi)), zhigh.at[0])
    zero(no(both(y_hi, z_hi)), zhigh.at[9])

    lane = lax.broadcasted_iota(jnp.int32, (8, 128), 1)
    sub = lax.broadcasted_iota(jnp.int32, (8, 128), 0)
    slot_of = ((lane + 2) & 127) >> 2
    quarter = lane & 3

    for h in range(2):
        own = field.at[8 * h + 2 : 8 * h + 10, 2:18]
        pltpu.make_async_copy(own, own, in_sem.at[h]).wait()

    def pack(bs):
        packed = {b: jnp.zeros((8, 128), F32) for b in bs}
        for s in range(32):
            mine = slot_of == s
            for b in bs:
                row = field[s // 2 + 2, 2 * b + s % 2 + 2]
                moved = pltpu.roll(row, 4 * s, 1) if s else row
                packed[b] = jnp.where(mine, moved, packed[b])
        for b in bs:
            zmid[b + 1] = packed[b]

    pack((0, 7))

    pl.semaphore_wait(barrier, greeted)

    tell(know.at[0], {"gx": gx - 1}, both(x_lo, gx <= half))
    for step in around:
        tell(know.at[1], near_to(*step))
    for d in range(1, nx):
        tell(know.at[3], {"gx": gx - d}, gx >= d)

    def remote(src, dst, send, recv, peer):
        return pltpu.make_async_remote_copy(
            src_ref=src, dst_ref=dst, send_sem=send, recv_sem=recv, device_id=peer, device_id_type=MESH
        )

    halos = [
        (zmid.at[1:9], zlow.at[1:9], (0, 1), 0),
        (zmid.at[1:9], zhigh.at[1:9], (0, -1), 0),
        (zmid.at[8], zlow.at[0], (1, 1), 1),
        (zmid.at[8], zhigh.at[0], (1, -1), 1),
        (zmid.at[1], zlow.at[9], (-1, 1), 1),
        (zmid.at[1], zhigh.at[9], (-1, -1), 1),
        (zmid.at[8], zmid.at[0], (1, 0), 1),
        (zmid.at[1], zmid.at[9], (-1, 0), 1),
    ]
    def send(halos):
        for src, dst, (dy, dz), i in halos:
            is_there = {(0, 1): z_hi, (0, -1): z_lo, (1, 0): y_hi, (-1, 0): y_lo}
            there = is_there.get((dy, dz))
            if there is None:
                there = both(is_there[dy, 0], is_there[0, dz])
            when(there, remote(src, dst, sent_sem.at[i // 2], came_sem.at[i], near_to(dy, dz)).start)
    y_halos = []
    for h in range(2):
        mine = pl.ds(8 * h + 2, 8)
        y_halos.append((field.at[mine, 16:18], field.at[mine, 0:2], (1, 0), 2 + h))
        y_halos.append((field.at[mine, 2:4], field.at[mine, 18:20], (-1, 0), 2 + h))
    send(halos[2:])
    send(y_halos)
    y_two, z_two = both(y_lo, y_hi), both(z_lo, z_hi)

    def flush(sem, tiles):
        for y_count in (1, 2):
            for z_count in (1, 2):
                n = tiles(y_count, z_count)
                ref = field.at[0, 0:n] if n <= 20 else field.at[0:4, 0 : n // 4] if n % 4 == 0 else field.at[0:2, 0 : n // 2]
                wait = pltpu.make_async_copy(ref, ref, sem).wait
                when(both(y_two if y_count == 2 else no(y_two), z_two if z_count == 2 else no(z_two)), wait)

    x_down = remote(
        field.at[2:4, 2:18], field.at[18:20, 2:18], sent_sem.at[2], came_sem.at[4], {"gx": gx - 1}
    )
    x_up = remote(
        field.at[16:18, 2:18], field.at[0:2, 2:18], sent_sem.at[3], came_sem.at[5], {"gx": gx + 1}
    )
    when(x_lo, x_down.start)
    when(soon, x_up.start)
    pack(range(1, 7))
    send(halos[:2])

    labels.wait()
    starts.wait()
    outer[...] = shell[...] >> 5
    inner[...] = shell[...] & 31
    first = jnp.broadcast_to(onsets[pl.ds(gy // 4, 1), :], (8, 128))
    first = pltpu.roll(first, lax.rem(128 - 32 * lax.rem(gy, 4), 128), 1)
    first = jnp.where(lane < 32, first, 0)
    first = first + pltpu.roll(first, 32, 1)
    first = first + pltpu.roll(first, 64, 1)

    signs = jnp.where(sub < 4, 1.0 / 24.0, -1.0 / 24.0).astype(F32)
    minus = -signs

    def shifts(f):
        return (pltpu.roll(f, k, 1) for k in (127, 126, 1, 2))

    def slope(up1, up2, down1, down2):
        d = (up1 - down1) * (8.0 / 144.0) - (up2 - down2) * (1.0 / 144.0)
        return pltpu.roll(d, 4, 0)

    def stars(x, y):
        near = (field[x + 1, y + 2] + field[x + 3, y + 2]) + (field[x + 2, y + 1] + field[x + 2, y + 3])
        far = (field[x, y + 2] + field[x + 4, y + 2]) + (field[x + 2, y] + field[x + 2, y + 4])
        return (16.0 * near - far) * signs

    def along_z(xs, whole):
        for x in xs:
            for y in range(16):
                f = field[x + 2, y + 2]
                up1, up2, down1, down2 = shifts(f)
                firsts[x, y + 2] = slope(up1, up2, down1, down2)
                bend = 16.0 * (up1 + down1) - (up2 + down2)
                value = (bend + 30.0 * f) * minus
                if whole and 2 <= y < 14:
                    value = value + stars(x, y)
                seconds[x, y] = value
        return 0

    lax.fori_loop(0, 3, lambda i, _: along_z([4 * i + 2 + j for j in range(4)], True), 0)
    lax.fori_loop(0, 2, lambda i, _: along_z([14 * i, 14 * i + 1], False), 0)

    when(late, lambda: pl.semaphore_wait(know.at[0], 1))
    when(late, x_up.start)

    flush(came_sem.at[0], lambda y, z: 8 * z)

    pl.semaphore_wait(know.at[1], 8)
    for dy, dz in around:
        tell(know.at[2], near_to(2 * dy, 2 * dz))

    even = (slot_of & 1) == 0
    at_end = jnp.logical_or(lane < 2, lane >= 126)
    turns = {}

    def turn(b):
        wrong = jnp.where(quarter >= 2, zlow[b], zhigh[b]) - zmid[b]
        near = jnp.where(
            quarter == 0, pltpu.roll(wrong, 1, 1), jnp.where(quarter == 3, pltpu.roll(wrong, 127, 1), 0.0)
        )
        far = jnp.where(quarter < 2, pltpu.roll(wrong, 2, 1), pltpu.roll(wrong, 126, 1))
        error = far - 8.0 * near
        error = jnp.where(quarter < 2, error, -error)
        turns[b] = (error, pltpu.roll(error, 124, 1), pltpu.roll(error, 4, 1), 16.0 * near - far)

    def mend(b):
        (before, before_up, _, _), (_, up, down, bend), (after, _, after_down, _) = (
            turns[b - 1],
            turns[b],
            turns[b + 1],
        )
        step1 = jnp.where(even, up - before_up, after_down - down)
        mixed = 8.0 * step1 - (after - before)
        fix = bend * minus - pltpu.roll(mixed, 4, 0) * (1.0 / 144.0)
        for s in range(32):
            x, y = s // 2, 2 * b - 2 + s % 2
            end = pltpu.roll(fix, 128 - 4 * s, 1) if s else fix
            seconds[x, y] = seconds[x, y] + jnp.where(at_end, end, 0.0)

    for b in range(1, 9):
        turn(b)
    for b in range(2, 8):
        mend(b)

    step_of = sub & 3
    uz = (lane + gz * 128).astype(F32)
    uz = (uz + 0.5) / (nz * 128) - 0.5
    uz2 = (uz * uz + 0.05) * 0.0625

    def rows(xs, ys, whole=False):
        lefts, rights = [], []
        for x in xs:
            ux = (x + gx * 16).astype(F32)
            ux = (ux + 0.5) / (nx * 16) - 0.5
            ux2 = uz2 + ux * ux * 0.0625
            for y in ys:
                mixed = 8.0 * (firsts[x, y + 3] - firsts[x, y + 1]) - (firsts[x, y + 4] - firsts[x, y])
                value = seconds[x, y] - mixed
                if not whole:
                    value = value + stars(x, y)
                psi_out[x, y] = value
                news = value + jnp.where(step_of >= 1, pltpu.roll(value, 1, 0), 0.0)
                news = news + jnp.where(step_of >= 2, pltpu.roll(news, 2, 0), 0.0)
                power = news * news
                power = power + pltpu.roll(power, 4, 0)
                uy = (gy * 16 + y).astype(F32)
                uy = (uy + 0.5) / (ny * 16) - 0.5
                flux = power * (ux2 + uy * uy * 0.0625)
                high = flux.astype(jnp.bfloat16).astype(F32)
                split = jnp.where(sub < 4, high, flux - high)
                high_label = jnp.broadcast_to(outer[x, pl.ds(y, 1), :], (8, 128))
                low_label = jnp.broadcast_to(inner[x, pl.ds(y, 1), :], (8, 128))
                lefts.append(
                    jnp.concatenate([jnp.where(high_label == k, split, 0.0) for k in range(8)], axis=0)
                )
                rights.append(
                    jnp.concatenate(
                        [jnp.where(low_label == sub + 8 * j, 1.0, 0.0).astype(F32) for j in range(4)], axis=0
                    )
                )
        left = jnp.concatenate(lefts, axis=1)
        right = jnp.concatenate(rights, axis=1)
        return lax.dot_general(left, right, (((1,), (1,)), ((), ())), preferred_element_type=F32)

    total = lax.fori_loop(
        0,
        2,
        lambda i, t: t + rows([6 * i + 2 + j for j in range(6)], range(2, 14), True),
        jnp.zeros((64, 32), F32),
    )
    binned[...] = jnp.zeros((64, 128), F32)
    binned[:, 0:32] = total

    def x_rows():
        when(x_hi, x_down.wait_recv)
        when(x_lo, x_up.wait_recv)
        binned[:, 0:32] += rows((0, 1, 14, 15), range(2, 14))

    x_last = jnp.logical_or(gx == half - 1, gx == half)

    def y_rows():
        flush(came_sem.at[1], lambda y, z: y * (z + 1))
        flush(came_sem.at[2], lambda y, z: 16 * y)

        def y_ends(xs):
            for x in xs:
                for y in (0, 1, 18, 19):
                    up1, up2, down1, down2 = shifts(field[x + 2, y])
                    firsts[x, y] = slope(up1, up2, down1, down2)

        y_ends(range(8))
        for b in (0, 1, 2, 7, 8, 9):
            turn(b)
        for b in (1, 8):
            mend(b)
        binned[:, 0:32] += rows(range(2, 8), (0, 1, 14, 15))
        flush(came_sem.at[3], lambda y, z: 16 * y)
        y_ends(range(8, 16))
        binned[:, 0:32] += rows(range(8, 14), (0, 1, 14, 15))

    def in_turn(i, _):
        x_now = (i == 0) != x_last
        when(x_now, x_rows)
        when(no(x_now), y_rows)
        return 0

    lax.fori_loop(0, 2, in_turn, 0)

    binned[:, 0:32] += rows((0, 1, 14, 15), (0, 1, 14, 15))

    pl.semaphore_wait(know.at[2], 8)

    def by_step(x, moves):
        moved = x
        for t in range(1, 4):
            moved = jnp.where(step_of == t, pltpu.roll(x, moves[t], 1), moved)
        return moved

    for k in range(8):
        spread = by_step(binned[8 * k : 8 * k + 8, :], (0, 32, 64, 96))
        parts[k] = jnp.sum(spread, axis=0, keepdims=True)

    offsets = [(dy, dz) for dy in range(ny) for dz in range(nz) if dy or dz]
    offsets.sort(key=lambda o: -(min(o[0], ny - o[0]) + min(o[1], nz - o[1]) / 2))
    for i, (dy, dz) in enumerate(offsets):
        peer = near_to(dy, dz)
        remote(parts.at[peer.get("gy", gy)], got.at[i], sent_sem.at[4], came_sem.at[6], peer).start()

    pltpu.make_async_copy(got, got, came_sem.at[6]).wait()
    sums = [parts[gy]] + [got[i] for i in range(len(offsets))]
    while len(sums) > 1:
        sums = [a + b for a, b in zip(sums[::2], sums[1::2])]
    value = sums[0]

    summed[0] = value
    when(x_hi, lambda: pl.semaphore_wait(know.at[3], nx - 1 - gx))
    for d in reversed(range(1, nx)):
        copy = remote(summed.at[0], got_x.at[d - 1], sent_sem.at[5], came_sem.at[7], {"gx": gx + d})
        when(gx + d < nx, copy.start)
    for n in range(1, nx):
        when(gx == n, pltpu.make_async_copy(got_x.at[0:n], got_x.at[0:n], came_sem.at[7]).wait)
    for d in range(1, nx):
        value = value + jnp.where(gx >= d, got_x[d - 1], 0.0)

    value = jnp.broadcast_to(value, (8, 128))
    value = jnp.where((lane >> 5) >= first, value, 0.0)
    value = value * (0.25 * 256 / (nx * 16 * ny * 16 * nz * 128))
    steps = [pltpu.roll(value, lax.rem(256 - 32 * t - 4 * gz, 128), 1) for t in range(4)]
    value = steps[0]
    for t in range(1, 4):
        value = value + jnp.where(sub >= t, steps[t], 0.0)
    energy_out[0] = value[0:4, 0:4]

    def left(i, ref):
        pltpu.make_async_copy(ref, ref, sent_sem.at[i]).wait()

    flush(sent_sem.at[0], lambda y, z: 8 * z + y * (z + 1))
    flush(sent_sem.at[1], lambda y, z: 32 * y)
    when(x_lo, x_down.wait_send)
    when(x_hi, x_up.wait_send)
    left(4, got)
    for n in range(1, nx):
        when(gx == nx - 1 - n, lambda n=n: left(5, got_x.at[0:n]))


def write(psi, energy, psi_out, energy_out, sem):
    for c in range(CT):
        for h in range(4):
            mine = pl.ds(4 * h, 4)
            pltpu.make_async_copy(psi.at[mine, :, c], psi_out.at[c, mine], sem.at[0]).start()
    small = pltpu.make_async_copy(energy, energy_out, sem.at[1])
    small.start()
    pltpu.make_async_copy(psi_out, psi_out, sem.at[0]).wait()
    small.wait()


def solution(mesh):
    sizes = tuple(mesh.shape[a] for a in ("gx", "gy", "gz"))
    vmem = pl.BlockSpec(memory_space=pltpu.VMEM)
    hbm = pl.BlockSpec(memory_space=pltpu.HBM)

    def body(strain, cell_shell_index, onset_step):
        psi, energy = pl.pallas_call(
            lambda *refs: kernel(sizes, *refs),
            out_shape=(pltpu.VMEM((16, 16, 8, 128), F32), pltpu.VMEM((1, 4, 4), F32)),
            in_specs=[hbm] * 3,
            out_specs=(vmem, vmem),
            scratch_shapes=[
                pltpu.VMEM((20, 20, 8, 128), F32),
                pltpu.VMEM((16, 16, 128), jnp.int32),
                pltpu.VMEM((2, 128), jnp.int32),
                pltpu.VMEM((10, 8, 128), F32),
                pltpu.VMEM((10, 8, 128), F32),
                pltpu.VMEM((10, 8, 128), F32),
                pltpu.VMEM((16, 16, 128), jnp.int32),
                pltpu.VMEM((16, 16, 128), jnp.int32),
                pltpu.VMEM((16, 20, 8, 128), F32),
                pltpu.VMEM((16, 16, 8, 128), F32),
                pltpu.VMEM((64, 128), F32),
                pltpu.VMEM((8, 1, 128), F32),
                pltpu.VMEM((63, 1, 128), F32),
                pltpu.VMEM((7, 1, 128), F32),
                pltpu.VMEM((1, 1, 128), F32),
                pltpu.SemaphoreType.DMA((4,)),
                pltpu.SemaphoreType.DMA((6,)),
                pltpu.SemaphoreType.DMA((8,)),
                pltpu.SemaphoreType.REGULAR((4,)),
            ],
            compiler_params=pltpu.CompilerParams(collective_id=0, has_side_effects=True),
        )(strain.reshape(8, 16, 16, 128), cell_shell_index, onset_step.reshape(2, 128))
        psi_four, energy = pl.pallas_call(
            write,
            out_shape=(
                jax.ShapeDtypeStruct((8, 16, 16, 128), F32),
                jax.ShapeDtypeStruct((1, 4, 4), F32),
            ),
            in_specs=[vmem] * 2,
            out_specs=(hbm, hbm),
            scratch_shapes=[pltpu.SemaphoreType.DMA((2,))],
        )(*(pltpu.with_memory_space_constraint(a, pltpu.VMEM) for a in (psi, energy)))
        return psi_four.reshape(strain.shape), energy

    placed = (P(None, None, "gx", "gy", "gz"), P("gx", "gy", "gz"), P())
    return jax.shard_map(
        body,
        mesh=mesh,
        in_specs=placed,
        out_specs=(P(None, None, "gx", "gy", "gz"), P("gx", None, ("gy", "gz"))),
        check_vma=False,
    )
```
